32 devices in a mesh: slab: 8 (over z, y), md: 4 (over x, core).
Axes of the slice: x: 2, y: 2, z: 4, core: 2. Of those that a mesh axis runs over, the one named last changes fastest.
Arguments:
- populations: float32 [19, 16, 256, 128], P(None, 'slab', 'md'), may hold values from 0.02 to 0.1
- relax: float32 [16, 256, 128], P('slab', 'md'), may hold values from 0.8 to 1.8
- owners: int32 [16, 256, 2], P('slab', 'md'), may hold values from 0 to 31, all different within a row; in each aligned block of 64 rows (0 to 63, 64 to 127, ..., all dimensions but the last counted through in order) at most 8 rows name the same one
- positions: float32 [3, 32768], P(None, ('slab', 'md')), may hold values from 0 to 3
- velocities: float32 [3, 32768], P(None, ('slab', 'md')), may hold values from -5 to 5
- neighbours: int32 [32768, 64], P(('slab', 'md')), may hold values from 0 to 1023
- atom_slots: int32 [32768], P(('slab', 'md')), may hold values from 0 to 511
Outputs:
- populations_out: float32 [19, 16, 256, 128], P(None, 'slab', 'md')
- positions_out: float32 [3, 32768], P(None, ('slab', 'md'))
- velocities_out: float32 [3, 32768], P(None, ('slab', 'md'))
- cell_moments: float32 [4, 16, 256], P(None, 'slab', 'md')
The draws below stay inside these ranges and needn't reach their ends.
Inputs may be any that keep to these rules, and one draw needn't show every extreme that they name: The 64 entries of one z position on one device name any owner at most 8 times in each column k and across k; the 2 owners of one cell differ. `neighbours`: entries index atoms of the same subdomain's block of 1024 atoms; an atom that lists itself is padding.
All inputs are finite; a program needn't handle non-finite values.
Results may differ from the reference program's by a relative error of at most 0.0003.
Values sent between devices are 32-bit elements; how exact they have to be, the bound alone decides.
A program may use at most 64 MiB of HBM per device.

```python
import math
import jax
import jax.numpy as jnp
import numpy as np
from jax import lax

CZ = 2
CX = 64
NY = 128
ATOMS = 1024
NBR = 64
TOP = 2
LB_STEPS = 4
MD_STEPS = 5
NZ = 16
NX = 256
ATOMS_ALL = 32768
MOST = 8
CAP = 16
SLOTS = 512
N_SLAB = 8
N_MD = 4
DEVICES = 32


def plant(values, own_key, smallest, top_value):
    longest = values.shape.index(max(values.shape))
    spots = []
    for shift in (0, 1):
        where = [jax.random.randint(jax.random.fold_in(own_key, axis), (), 0, length) for axis, length in enumerate(values.shape)]
        where[longest] = (where[longest] + shift) % values.shape[longest]
        spots.append(tuple(where))
    return values.at[spots[0]].set(smallest).at[spots[1]].set(top_value)


def block_scale(stream_key, shape, cuts, low, high):
    def one(position, shards_of):
        steps = jax.random.uniform(jax.random.fold_in(jax.random.fold_in(stream_key, 6), position), (shards_of,), jnp.float32, low / len(cuts), high / len(cuts))
        return jnp.repeat(jnp.exp(steps), shape[position] // shards_of).reshape((-1,) + (1,) * (len(shape) - position - 1))

    gain = one(*cuts[0])
    for cut in cuts[1:]:
        gain = gain * one(*cut)
    return gain


def deal_out(key, own, number, rows, count, top, bound, lean):
    sequence = jax.random.permutation(key, count)
    packed, common = load_shares(count, rows * top, bound, lean, True), load_shares(count, rows * top, bound, lean, False)
    places = jnp.arange(count)

    def named(lengths, turn):
        used = int((lengths > 0).sum())
        fixed = max(1, used // 4)
        moved = fixed + (places - fixed + turn * (used - fixed)) % max(1, count - fixed)
        return jnp.zeros((count,), jnp.int32).at[sequence[jnp.where(places < fixed, places, moved)]].set(jnp.asarray(lengths, jnp.int32))

    lengths = jnp.where(number % 4 == 0, named(packed, number // 4), named(common, number - number // 4 - 1))
    mixed = jax.random.permutation(jax.random.fold_in(own, 3), count)
    giver, taker = mixed[0:count // 2 * 2:2], mixed[1:count // 2 * 2:2]
    slack = jnp.minimum(lengths[giver] - 1, bound - lengths[taker]) // 2
    slack = jnp.where((giver == sequence[0]) | (taker == sequence[0]) | (lengths[taker] == 0), 0, jnp.maximum(slack, 0))
    moved = jax.random.randint(jax.random.fold_in(own, 4), (count // 2,), 0, 1 << 20) % (slack + 1)
    lengths = lengths.at[giver].add(-moved).at[taker].add(moved)
    items = jnp.searchsorted(jnp.cumsum(lengths), jnp.arange(rows * top), side="right").astype(jnp.int32)
    listing = items.reshape(top, rows).T
    listing = listing[jax.random.permutation(jax.random.fold_in(own, 1), rows)]
    turn = jax.random.randint(jax.random.fold_in(own, 2), (rows, 1), 0, top)
    return jnp.take_along_axis(listing, (jnp.arange(top)[None, :] + turn) % top, axis=1)


def load_shares(amount, total, reach, skew, full):
    loads = [(1 << 20) // math.isqrt(grade ** skew) + 1 for grade in range(1, amount + 1)]
    largest = reach if full else min(reach, max(-(-total // amount), total * loads[0] // sum(loads)))
    least = 1 if total - largest >= amount - 1 else 0
    counts, spare = [largest] + [least] * (amount - 1), total - largest - least * (amount - 1)
    while spare > 0:
        movable = [i for i in range(1, amount) if counts[i] < largest] or [i for i in range(1, amount) if counts[i] < reach]
        whole, budget = sum([loads[i] for i in movable]), spare
        for i in movable:
            more = min(reach - counts[i], max(1, budget * loads[i] // whole), spare)
            counts[i] = counts[i] + more
            spare = spare - more
    return np.array(counts)


def bell_draw(rng, dims, deviation, limit, cuts=(), kind=jnp.bfloat16):
    drawn = deviation * jax.random.normal(rng, dims, jnp.float32)
    if cuts:
        drawn = drawn * block_scale(rng, dims, cuts, -0.22, 0.18)
    return jnp.clip(drawn, -limit, limit).astype(kind)


def setup_inputs(seed: int = 0) -> dict:
    keys = jax.random.split(jax.random.key(seed), 8)
    populations = jnp.clip(0.02 + 0.08 * jax.random.uniform(keys[0], (19, NZ, NX, NY), jnp.float32) ** block_scale(keys[0], (19, NZ, NX, NY), ((1, 8), (2, 4)), -0.2, 0.2), 0.02, 0.1)
    relax = jnp.clip(jnp.exp(math.log(1.8) - 0.8109302 * jax.random.uniform(keys[1], (NZ, NX, NY), jnp.float32) ** block_scale(keys[1], (NZ, NX, NY), ((0, 8), (1, 4)), -0.2, 0.2)), 0.8, 1.8)
    owners_keys = jax.random.split(jax.random.fold_in(keys[2], 1), NZ * NX // CX)
    owners_turns = jax.random.permutation(jax.random.fold_in(keys[2], 3), NZ * NX // CX)
    owners = jax.vmap(lambda own, number: deal_out(jax.random.fold_in(keys[2], 2), own, number, CX, DEVICES, TOP, MOST, 2))(owners_keys, owners_turns).reshape((NZ, NX, TOP))
    positions = jnp.clip(3.0 * jax.random.uniform(keys[3], (3, ATOMS_ALL), jnp.float32) ** block_scale(keys[3], (3, ATOMS_ALL), ((1, 32),), -0.2, 0.2), 0.0, 3.0)
    velocities = bell_draw(keys[4], (3, ATOMS_ALL), 1.0, 5.0, ((1, 32),), jnp.float32)
    neighbours = plant(jax.random.randint(keys[5], (ATOMS_ALL, NBR), 0, ATOMS), jax.random.fold_in(keys[5], 1), 0, ATOMS - 1).astype(jnp.int32)
    atom_slots = plant(jax.random.randint(keys[6], (ATOMS_ALL,), 0, SLOTS), jax.random.fold_in(keys[6], 1), 0, SLOTS - 1).astype(jnp.int32)
    return dict(populations=populations, relax=relax, owners=owners, positions=positions, velocities=velocities, neighbours=neighbours, atom_slots=atom_slots)


lattice_dirs = [(0, 0, 0), (1, 0, 0), (-1, 0, 0), (0, 1, 0), (0, -1, 0), (0, 0, 1), (0, 0, -1),
                (1, 1, 0), (-1, -1, 0), (1, -1, 0), (-1, 1, 0), (1, 0, 1), (-1, 0, -1), (1, 0, -1),
                (-1, 0, 1), (0, 1, 1), (0, -1, -1), (0, 1, -1), (0, -1, 1)]
lattice_weights = [1.0 / 3.0] + [1.0 / 18.0] * 6 + [1.0 / 36.0] * 12
velocity_scale = 10.0
pair_strength = 0.5
friction = 2.0
time_step = 0.1


def velocity(f, density):
    comps = []
    for axis_id in range(3):
        total = jnp.zeros_like(density)
        for index, direction in enumerate(lattice_dirs):
            if direction[axis_id] != 0:
                total = total + direction[axis_id] * f[index]
        comps.append(total / density)
    return comps


def collide(f, relax):
    density = jnp.sum(f, axis=0)
    vel_x, vel_y, vel_z = velocity(f, density)
    usq = vel_x * vel_x + vel_y * vel_y + vel_z * vel_z
    result = []
    for index, direction in enumerate(lattice_dirs):
        along = direction[0] * vel_x + direction[1] * vel_y + direction[2] * vel_z
        equil = lattice_weights[index] * density * (1.0 + 3.0 * along + 4.5 * along * along - 1.5 * usq)
        result.append(f[index] - relax * (f[index] - equil))
    return result


def md_run(pos, vel, nbr, slots, recv):
    target = recv[slots]
    goal = target[:, :3].T
    dens = target[:, 3]
    for step in range(MD_STEPS):
        gap = pos[:, nbr] - pos[:, :, None]
        weight = jnp.exp(-0.5 * jnp.sum(gap * gap, axis=0))
        force = pair_strength * jnp.sum(gap * weight[None], axis=2) + friction * dens[None, :] * (goal - vel)
        vel = vel + time_step * force
        pos = pos + time_step * vel
    data = jnp.concatenate([vel, jnp.sum(vel * vel, axis=0, keepdims=True)], axis=0).T
    sums = jax.ops.segment_sum(data, slots, num_segments=recv.shape[0])
    count = jax.ops.segment_sum(jnp.ones(slots.shape, jnp.float32), slots, num_segments=recv.shape[0])
    return pos, vel, sums / jnp.maximum(count, 1.0)[:, None]


def reference(populations, relax, owners, positions, velocities, neighbours, atom_slots):
    f = populations
    for step in range(LB_STEPS):
        post = collide(f, relax)
        f = jnp.stack([jnp.roll(post[i], (c[2], c[0], c[1]), axis=(0, 1, 2)) for i, c in enumerate(lattice_dirs)])
    density = jnp.sum(f, axis=0)
    vel_x, vel_y, vel_z = velocity(f, density)
    targets = jnp.stack([jnp.mean(velocity_scale * vel_x, axis=2), jnp.mean(velocity_scale * vel_y, axis=2),
                         jnp.mean(velocity_scale * vel_z, axis=2), jnp.mean(density, axis=2)])
    devices = N_SLAB * N_MD
    entries = CZ * CX * TOP
    tgt_dev = targets.reshape(4, N_SLAB, CZ, N_MD, CX).transpose(1, 3, 0, 2, 4).reshape(devices, 4, CZ * CX)
    vals = jnp.repeat(tgt_dev, TOP, axis=2).transpose(0, 2, 1)
    own = owners.reshape(N_SLAB, CZ, N_MD, CX, TOP).transpose(0, 2, 1, 3, 4).reshape(devices, entries)
    labels = jnp.arange(devices, dtype=jnp.int32)

    def ranks_of(row):
        onehot = (row[:, None] == labels[None, :]).astype(jnp.int32)
        before = jnp.cumsum(onehot, axis=0) - onehot
        return jnp.sum(before * onehot, axis=1).astype(jnp.int32)

    rank = lax.map(ranks_of, own)
    slot = (labels[:, None] * CAP + rank).astype(jnp.int32)
    pos_dev = positions.reshape(3, devices, ATOMS).transpose(1, 0, 2)
    vel_dev = velocities.reshape(3, devices, ATOMS).transpose(1, 0, 2)
    nbr_dev = neighbours.reshape(devices, ATOMS, NBR)
    slot_dev = atom_slots.reshape(devices, ATOMS)

    def per_owner(back, inputs):
        owner_id, pos, vel, nbr, slots = inputs
        hit = own == owner_id
        where_to = jnp.where(hit, slot, SLOTS).astype(jnp.int32)
        recv = jnp.zeros((SLOTS, 4), jnp.float32).at[where_to].set(vals, mode="drop")
        pos, vel, moms = md_run(pos, vel, nbr, slots, recv)
        back = back + jnp.where(hit[:, :, None], moms[slot], 0.0)
        return back, (pos, vel)

    back, (pos_out, vel_out) = lax.scan(per_owner, jnp.zeros((devices, entries, 4), jnp.float32),
                                        (labels, pos_dev, vel_dev, nbr_dev, slot_dev))
    summed = back.reshape(devices, CZ * CX, TOP, 4).sum(axis=2).transpose(0, 2, 1)
    cell_moments = summed.reshape(N_SLAB, N_MD, 4, CZ, CX).transpose(2, 0, 3, 1, 4).reshape(4, NZ, NX)
    positions_out = pos_out.transpose(1, 0, 2).reshape(3, ATOMS_ALL)
    velocities_out = vel_out.transpose(1, 0, 2).reshape(3, ATOMS_ALL)
    return f, positions_out, velocities_out, cell_moments
```

```python
import contextlib
import functools

import jax
import jax.numpy as jnp
from jax import lax
from jax.experimental import pallas as pl
from jax.experimental.pallas import tpu as pltpu
from jax.sharding import PartitionSpec as P

LB_STEPS = 4
MD_STEPS = 5

ORDER = [11, 14, 5, 15, 18, 12, 13, 6, 16, 17, 0, 1, 2, 3, 4, 7, 8, 9, 10]
lattice_dirs = [
    (0, 0, 0),
    (1, 0, 0),
    (-1, 0, 0),
    (0, 1, 0),
    (0, -1, 0),
    (0, 0, 1),
    (0, 0, -1),
    (1, 1, 0),
    (-1, -1, 0),
    (1, -1, 0),
    (-1, 1, 0),
    (1, 0, 1),
    (-1, 0, -1),
    (1, 0, -1),
    (-1, 0, 1),
    (0, 1, 1),
    (0, -1, -1),
    (0, 1, -1),
    (0, -1, 1),
]
DIRS = [lattice_dirs[i] for i in ORDER]
FACES = [[p for p in range(19) if DIRS[p][0] == 1], [p for p in range(19) if DIRS[p][0] == -1]]
velocity_scale = 10.0
pair_strength = 0.5
friction = 2.0
time_step = 0.1
MESH = pl.DeviceIdType.MESH


def parts_of(cx):
    edges = list(range(0, cx + 1, 8))
    parts = list(zip(edges[:-1], edges[1:]))
    order = []
    while parts:
        order.append(parts.pop(0))
        if parts:
            order.append(parts.pop())
    return order


def mark(name):
    return contextlib.nullcontext()


def total_of(terms):
    terms = list(terms)
    while len(terms) > 1:
        terms = [a + b for a, b in zip(terms[::2], terms[1::2])] + (
            [terms[-1]] if len(terms) % 2 else []
        )
    return terms[0]


def fields(f):
    density = total_of(f)
    inverse = 1.0 / density
    vel = []
    for axis in range(3):
        plus = total_of(f[p] for p in range(19) if DIRS[p][axis] == 1)
        minus = total_of(f[p] for p in range(19) if DIRS[p][axis] == -1)
        vel.append((plus - minus) * inverse)
    return density, vel


def collided(f, relax):
    density, (vx, vy, vz) = fields(f)
    base = 1.0 - 1.5 * (vx * vx + vy * vy + vz * vz)
    keep = 1.0 - relax
    scale = relax * density
    result = [None] * 19
    for p, c in enumerate(DIRS):
        if result[p] is not None:
            continue
        size = sum(abs(e) for e in c)
        if size == 0:
            result[p] = keep * f[p] + (scale * (1.0 / 3.0)) * base
            continue
        along = total_of(v if e == 1 else -v for e, v in zip(c, (vx, vy, vz)) if e)
        weight = scale * (1.0 / 18.0 if size == 1 else 1.0 / 36.0)
        even = weight * (base + 4.5 * (along * along))
        odd = weight * (3.0 * along)
        q = DIRS.index(tuple(-e for e in c))
        result[p] = keep * f[p] + (even + odd)
        result[q] = keep * f[q] + (even - odd)
    return result


def lane_gather(table, index):
    return jnp.take_along_axis(table, index, axis=1, mode="promise_in_bounds")


def thirds(value):
    parts = []
    for _ in range(3):
        piece = value.astype(jnp.bfloat16).astype(jnp.float32)
        parts.append(piece)
        value = value - piece
    return parts


def by_hits(data, hits, dims):
    return lax.dot_general(
        data.astype(jnp.bfloat16), hits, (dims, ((), ())), preferred_element_type=jnp.float32
    )


def coupled_kernel(
    n_slab,
    n_md,
    f_hbm,
    relax_hbm,
    own_hbm,
    pos_hbm,
    vel_hbm,
    nbr_hbm,
    slots_hbm,
    out_ref,
    pos_out,
    vel_out,
    cell_out,
    f_ref,
    relax_ref,
    own_ref,
    pos_ref,
    vel_ref,
    nbr_ref,
    slots_ref,
    load_sem,
    post,
    rows_out,
    rows_in,
    mean_ref,
    at,
    pull,
    data,
    hits,
    placed,
    tgt,
    table,
    blocks_out,
    blocks_in,
    send,
    recv,
    swap_send,
    swap_recv,
):
    cz, cx, ny = relax_ref.shape
    top_z = cz - 1
    cells = cz * cx
    entries, atoms = nbr_ref.shape
    groups = atoms // 128
    slot_count = hits.shape[0]
    devices = n_slab * n_md
    cap = slot_count // devices
    parts = parts_of(cx)
    chunks = len(parts)
    outer = [[low for low, _ in parts].index(0), [high for _, high in parts].index(cx)]
    slab, md = lax.axis_index("slab"), lax.axis_index("md")
    me = slab * n_md + md

    def wrapped(value, size):
        return jnp.where(value >= size, value - size, value)

    above, below = wrapped(slab + 1, n_slab), wrapped(slab + n_slab - 1, n_slab)
    right, left = wrapped(md + 1, n_md), wrapped(md + n_md - 1, n_md)
    barrier = pltpu.get_barrier_semaphore()

    def peer_of(k):
        return wrapped(slab + k // n_md, n_slab), wrapped(md + k % n_md, n_md)

    def source_of(k):
        return wrapped(slab + n_slab - k // n_md, n_slab), wrapped(md + n_md - k % n_md, n_md)

    for k in range(1, devices):
        pl.semaphore_signal(barrier, inc=1, device_id=peer_of(k), device_id_type=MESH)

    loads = []

    def fetch(src, dst):
        made = pltpu.make_async_copy(src, dst, load_sem.at[len(loads)])
        made.start()
        loads.append(made)
        return made

    f_parts = []
    for low, high in parts:
        here = pl.ds(low, high - low)
        f_parts.append(fetch(f_hbm.at[:, :, here, :], f_ref.at[:, :, here, :]))
        if len(f_parts) == 1:
            relax_part = fetch(relax_hbm, relax_ref)
    pos_parts = [fetch(pos_hbm, pos_ref), fetch(vel_hbm, vel_ref), fetch(nbr_hbm, nbr_ref)]
    slots_part = fetch(slots_hbm, slots_ref)
    own_part = fetch(own_hbm, own_ref)

    def load(step, z, x0):
        if step == 0:
            return [f_ref[ORDER[p], z, pl.ds(x0, 8), :] for p in range(19)]
        return [
            post[step - 1, p, z + 1 - c[2], pl.ds(x0 + (8 - c[0]), 8), :]
            for p, c in enumerate(DIRS)
        ]

    def collide_chunk(step, z, part):
        for x0 in range(*parts[part], 8):
            done = collided(load(step, z, x0), relax_ref[z, pl.ds(x0, 8), :])
            for p, c in enumerate(DIRS):
                value = done[p] if c[1] == 0 else pltpu.roll(done[p], c[1] % ny, axis=1)
                post[step, p, z + 1, pl.ds(x0 + 8, 8), :] = value

    copies = {}

    def copy(step, slot, src, dst, peer):
        made = pltpu.make_async_remote_copy(
            src_ref=src,
            dst_ref=dst,
            send_sem=send.at[step, slot],
            recv_sem=recv.at[step, slot],
            device_id=peer,
            device_id_type=MESH,
        )
        made.start()
        copies[step, slot] = [made, False]

    def arrive(step, slot):
        made = copies[step, slot]
        if not made[1]:
            made[1] = True
            made[0].wait_recv()
            return True
        return False

    def edge_slot(rising, side):
        return 2 + 2 * int(rising) + side

    def plane_slot(rising, part):
        return 6 + chunks * int(rising) + part

    def save_face(step, z, side):
        row = (7 + cx, 8)[side]
        for j, p in enumerate(FACES[side]):
            rows_out[step, side, z, j, :] = post[step, p, z + 1, row, :]

    def send_face(step, side):
        copy(
            step,
            side,
            rows_out.at[step, side],
            rows_in.at[step, side, pl.ds(1, cz)],
            (slab, (right, left)[side]),
        )

    def send_edge(step, rising, side):
        z, slot, peer = (top_z, 0, above) if rising else (0, cz + 1, below)
        copy(
            step,
            edge_slot(rising, side),
            rows_out.at[step, side, z],
            rows_in.at[step, side, slot],
            (peer, (right, left)[side]),
        )

    def send_plane(step, rising, part):
        z, slot, peer = (top_z, 0, above) if rising else (0, cz + 1, below)
        span = pl.ds(0 if rising else 5, 5)
        low, high = parts[part]
        here = pl.ds(8 + low, high - low)
        copy(
            step,
            plane_slot(rising, part),
            post.at[step, span, z + 1, here, :],
            post.at[step, span, slot, here, :],
            (peer, md),
        )

    def need(step, part, rising):
        for side in range(2):
            if part != outer[side]:
                continue
            row = (7, 8 + cx)[side]
            if arrive(step, side):
                for z in range(cz):
                    for j, p in enumerate(FACES[side]):
                        post[step, p, z + 1, row, :] = rows_in[step, side, z + 1, j, :]
            if arrive(step, edge_slot(not rising, side)):
                slot = cz + 1 if rising else 0
                sign = -1 if rising else 1
                for j, p in enumerate(FACES[side]):
                    if DIRS[p][2] == sign:
                        post[step, p, slot, row, :] = rows_in[step, side, slot, j, :]
        low, high = parts[part]
        for other in range(chunks):
            if parts[other][0] <= high and parts[other][1] >= low:
                arrive(step, plane_slot(not rising, other))

    def send_chunk(step, rising, part):
        z = top_z if rising else 0
        for side in range(2):
            if part == outer[1 - side]:
                save_face(step, z, side)
                send_edge(step, rising, side)
        send_plane(step, rising, part)

    def lattice_step(step):
        for part in range(chunks):
            if step == 0:
                f_parts[part].wait()
                if part == 0:
                    relax_part.wait()
            for rising in (True, False):
                if step:
                    with mark("need"):
                        need(step - 1, part, rising)
                with mark("collide"):
                    collide_chunk(step, top_z if rising else 0, part)
                if step or part:
                    send_chunk(step, rising, part)
            for z in range(1, top_z):
                collide_chunk(step, z, part)
                for side in range(2):
                    if part == outer[1 - side]:
                        save_face(step, z, side)
            if step == 0 and part == 0:
                with mark("barrier"):
                    pl.semaphore_wait(barrier, devices - 1)
                for rising in (True, False):
                    send_chunk(step, rising, part)
            for side in range(2):
                if part == outer[1 - side]:
                    send_face(step, side)

    def pair_forces():
        for g in range(groups):
            mine = [jnp.broadcast_to(at[c, pl.ds(g, 1), :], (8, 128)) for c in range(3)]
            sums = [jnp.zeros((8, 128), jnp.float32)] * 3
            for k in range(0, entries, 8):
                index = nbr_ref[pl.ds(k, 8), pl.ds(g * 128, 128)]
                lane, row = index & 127, index >> 7
                found = [None] * 3
                for h in range(groups):
                    pick = row == h
                    for c in range(3):
                        line = jnp.broadcast_to(at[c, pl.ds(h, 1), :], (8, 128))
                        value = lane_gather(line, lane)
                        found[c] = value if h == 0 else jnp.where(pick, value, found[c])
                gap = [found[c] - mine[c] for c in range(3)]
                weight = jnp.exp(-0.5 * (gap[0] * gap[0] + gap[1] * gap[1] + gap[2] * gap[2]))
                sums = [sums[c] + gap[c] * weight for c in range(3)]
            for c in range(3):
                pull[c, pl.ds(g, 1), :] = jnp.sum(sums[c], axis=0, keepdims=True)

    def prepare_particles():
        for part in pos_parts:
            part.wait()
        for g in range(groups):
            here = pl.ds(g * 128, 128)
            for c in range(3):
                at[c, pl.ds(g, 1), :] = pos_ref[pl.ds(c, 1), here]
                at[3 + c, pl.ds(g, 1), :] = vel_ref[pl.ds(c, 1), here]
        pair_forces()

    def prepare_hits():
        slots_part.wait()
        data[...] = jnp.ones(data.shape, jnp.float32)
        tgt[...] = jnp.zeros(tgt.shape, jnp.float32)
        table[...] = jnp.zeros(table.shape, jnp.float32)
        for g in range(groups):
            label = lax.broadcasted_iota(jnp.int32, (slot_count, 128), 0)
            same = label == slots_ref[pl.ds(g, 1), :]
            hits[:, pl.ds(g * 128, 128)] = jnp.where(same, 1.0, 0.0).astype(jnp.bfloat16)

    def prepare_routes():
        own_part.wait()
        top = own_ref.shape[1]
        owner = [
            jnp.concatenate([own_ref[z, pl.ds(k, 1), :] for z in range(cz)], axis=1)
            for k in range(top)
        ]
        label = lax.broadcasted_iota(jnp.int32, (devices, cells), 0)
        owned = [jnp.where(label == owner[k], 1.0, 0.0) for k in range(top)]
        earlier = lax.broadcasted_iota(jnp.int32, (cells, cells), 0) < lax.broadcasted_iota(
            jnp.int32, (cells, cells), 1
        )
        before = by_hits(
            total_of(owned), jnp.where(earlier, 1.0, 0.0).astype(jnp.bfloat16), ((1,), (0,))
        )
        start = (label * cap).astype(jnp.float32)
        place = lax.broadcasted_iota(jnp.int32, (slot_count, cells), 0).astype(jnp.float32)
        filled = jnp.zeros((slot_count, cells), jnp.float32)
        for k in range(top):
            spot = jnp.sum((before + start) * owned[k], axis=0, keepdims=True)
            filled = filled + jnp.where(place == spot, 1.0, 0.0)
            before = before + owned[k]
        placed[...] = filled.astype(jnp.bfloat16)

    def swap(turn, values, meanwhile):
        per = 128 // cap
        for d in range(devices):
            part = values[:, d // per * 128 : (d // per + 1) * 128]
            shift = (128 - d % per * cap) % 128
            blocks_out[turn, d] = part if shift == 0 else pltpu.roll(part, shift, axis=1)
        with mark("begin"):
            for k in sorted(range(1, devices), key=lambda k: -min(k // n_md, n_slab - k // n_md)):
                peer = peer_of(k)
                pltpu.make_async_remote_copy(
                    src_ref=blocks_out.at[turn, peer[0] * n_md + peer[1]],
                    dst_ref=blocks_in.at[turn, k],
                    send_sem=swap_send.at[turn],
                    recv_sem=swap_recv.at[turn],
                    device_id=peer,
                    device_id_type=MESH,
                ).start()
        blocks_in[turn, 0] = blocks_out[turn, me]
        meanwhile()
        everyone = pltpu.make_async_remote_copy(
            src_ref=blocks_out.at[turn, pl.ds(1, devices - 1)],
            dst_ref=blocks_in.at[turn, pl.ds(1, devices - 1)],
            send_sem=swap_send.at[turn],
            recv_sem=swap_recv.at[turn],
            device_id=(above, md),
            device_id_type=MESH,
        )
        with mark("landed"):
            everyone.wait_recv()
        zone = lax.broadcasted_iota(jnp.int32, (4, 128), 1) // cap
        lines = []
        for h in range(slot_count // 128):
            line = jnp.zeros((4, 128), jnp.float32)
            for j in range(per):
                source = h * per + j
                apart = wrapped(slab + n_slab - source // n_md, n_slab) * n_md + wrapped(
                    md + n_md - source % n_md, n_md
                )
                value = blocks_in[turn, apart]
                if j:
                    value = pltpu.roll(value, j * cap, axis=1)
                line = jnp.where(zone == j, value, line)
            lines.append(line)
        return lines, everyone.wait_send

    lattice_step(0)
    with mark("prep_part"):
        prepare_particles()
    lattice_step(1)
    with mark("hits"):
        prepare_hits()
    lattice_step(2)
    with mark("routes"):
        prepare_routes()
    for step in range(3, LB_STEPS):
        lattice_step(step)

    def finish_chunk(z, part):
        for x0 in range(*parts[part], 8):
            f = load(LB_STEPS, z, x0)
            for p in range(19):
                out_ref[ORDER[p], z, pl.ds(x0, 8), :] = f[p]
            density, vel = fields(f)
            for c, value in enumerate((*vel, density)):
                mean_ref[c, pl.ds(x0 + z * cx, 8), :] = value

    for part in range(chunks):
        for rising in (True, False):
            with mark("need_last"):
                need(LB_STEPS - 1, part, rising)
            finish_chunk(top_z if rising else 0, part)
        for z in range(1, top_z):
            finish_chunk(z, part)

    with mark("mean"):
        for c in range(4):
            scale = (velocity_scale if c < 3 else 1.0) / ny
            mean = jnp.sum(mean_ref[c].T, axis=0, keepdims=True) * scale
            for part, piece in enumerate(thirds(mean)):
                tgt[pl.ds(part * 4 + c, 1), :] = piece
        sums = by_hits(tgt[...], placed[...], ((1,), (1,)))

    def lattice_sent():
        for made, _ in copies.values():
            made.wait_send()

    with mark("swap0"):
        lines, sent_first = swap(0, sums[0:4] + sums[4:8] + sums[8:12], lattice_sent)

    slots = slots_ref[...]
    lane, row = slots & 127, slots >> 7
    goal = []
    for c in range(4):
        value = jnp.zeros((groups, 128), jnp.float32)
        for h, line in enumerate(lines):
            spread = jnp.broadcast_to(line[c : c + 1, :], (groups, 128))
            value = jnp.where(row == h, lane_gather(spread, lane), value)
        goal.append(value)
    rate = friction * goal[3]

    def advance():
        for c in range(3):
            vel = at[3 + c]
            force = pair_strength * pull[c] + rate * (goal[c] - vel)
            vel = vel + time_step * force
            at[3 + c] = vel
            at[c] = at[c] + time_step * vel

    def one_step(step, carry):
        with mark("pair"):
            pair_forces()
        with mark("advance"):
            advance()
        return carry

    advance()
    lax.fori_loop(1, MD_STEPS, one_step, 0)
    with mark("moments"):
        at[6] = at[3] * at[3] + at[4] * at[4] + at[5] * at[5]
        for c in range(4):
            for part, piece in enumerate(thirds(at[3 + c])):
                for g in range(groups):
                    data[pl.ds(part * 4 + c, 1), pl.ds(g * 128, 128)] = piece[g : g + 1, :]
        sums = by_hits(data[...], hits[...], ((1,), (1,)))
        moments = (sums[0:4] + sums[4:8] + sums[8:12]) / jnp.maximum(sums[12:13], 1.0)

    def put_particles():
        sent_first()
        for g in range(groups):
            here = pl.ds(g * 128, 128)
            for c in range(3):
                pos_out[pl.ds(c, 1), here] = at[c, pl.ds(g, 1), :]
                vel_out[pl.ds(c, 1), here] = at[3 + c, pl.ds(g, 1), :]

    with mark("swap1"):
        lines, sent_second = swap(1, moments, put_particles)
    for h, line in enumerate(lines):
        for part, piece in enumerate(thirds(line)):
            table[pl.ds(part * 4, 4), pl.ds(h * 128, 128)] = piece
    sums = by_hits(table[...], placed[...], ((1,), (0,)))
    picked = sums[0:4] + sums[4:8] + sums[8:12]
    for c in range(4):
        for z in range(cz):
            cell_out[c, pl.ds(z, 1), :] = picked[c : c + 1, z * cx : (z + 1) * cx]
    sent_second()


def on_device(populations, relax, owners, positions, velocities, neighbours, atom_slots):
    cz, cx, ny = relax.shape
    n_slab = lax.axis_size("slab")
    n_md = lax.axis_size("md")
    devices = n_slab * n_md
    top = owners.shape[2]
    cap = cz * max(2, 2 * cx * top // devices)
    slots = devices * cap
    atoms, entries = neighbours.shape
    groups = atoms // 128
    cells = cz * cx
    chunks = len(parts_of(cx))
    vmem = pl.BlockSpec(memory_space=pltpu.VMEM)
    hbm = pl.BlockSpec(memory_space=pltpu.HBM)
    dma = pltpu.SemaphoreType.DMA
    return pl.pallas_call(
        functools.partial(coupled_kernel, n_slab, n_md),
        out_shape=(
            jax.ShapeDtypeStruct(populations.shape, jnp.float32),
            jax.ShapeDtypeStruct(positions.shape, jnp.float32),
            jax.ShapeDtypeStruct(velocities.shape, jnp.float32),
            jax.ShapeDtypeStruct((4, cz, cx), jnp.float32),
        ),
        in_specs=[hbm] * 7,
        out_specs=(vmem,) * 4,
        scratch_shapes=[
            pltpu.VMEM(populations.shape, jnp.float32),
            pltpu.VMEM(relax.shape, jnp.float32),
            pltpu.VMEM((cz, top, cx), jnp.int32),
            pltpu.VMEM(positions.shape, jnp.float32),
            pltpu.VMEM(velocities.shape, jnp.float32),
            pltpu.VMEM((entries, atoms), jnp.int32),
            pltpu.VMEM((groups, 128), jnp.int32),
            dma((chunks + 6,)),
            pltpu.VMEM((LB_STEPS, 19, cz + 2, cx + 16, ny), jnp.float32),
            pltpu.VMEM((LB_STEPS, 2, cz, 8, ny), jnp.float32),
            pltpu.VMEM((LB_STEPS, 2, cz + 2, 8, ny), jnp.float32),
            pltpu.VMEM((4, cells, ny), jnp.float32),
            pltpu.VMEM((7, groups, 128), jnp.float32),
            pltpu.VMEM((3, groups, 128), jnp.float32),
            pltpu.VMEM((16, atoms), jnp.float32),
            pltpu.VMEM((slots, atoms), jnp.bfloat16),
            pltpu.VMEM((slots, cells), jnp.bfloat16),
            pltpu.VMEM((16, cells), jnp.float32),
            pltpu.VMEM((16, slots), jnp.float32),
            pltpu.VMEM((2, devices, 4, 128), jnp.float32),
            pltpu.VMEM((2, devices, 4, 128), jnp.float32),
            dma((LB_STEPS, 6 + 2 * chunks)),
            dma((LB_STEPS, 6 + 2 * chunks)),
            dma((2,)),
            dma((2,)),
        ],
        compiler_params=pltpu.CompilerParams(
            collective_id=0, has_side_effects=True, vmem_limit_bytes=67043328
        ),
        name="coupled",
    )(
        populations,
        relax,
        owners.transpose(0, 2, 1),
        positions,
        velocities,
        neighbours.T,
        atom_slots.reshape(groups, 128),
    )


def solution(mesh):
    return jax.shard_map(
        on_device,
        mesh=mesh,
        in_specs=(
            P(None, "slab", "md", None),
            P("slab", "md", None),
            P("slab", "md", None),
            P(None, ("slab", "md")),
            P(None, ("slab", "md")),
            P(("slab", "md"), None),
            P(("slab", "md")),
        ),
        out_specs=(
            P(None, "slab", "md", None),
            P(None, ("slab", "md")),
            P(None, ("slab", "md")),
            P(None, "slab", "md"),
        ),
        check_vma=False,
    )
```

```python
import contextlib
import functools

import jax
import jax.numpy as jnp
from jax import lax
from jax.experimental import pallas as pl
from jax.experimental.pallas import tpu as pltpu
from jax.sharding import PartitionSpec as P

LB_STEPS = 4
MD_STEPS = 5

ORDER = [11, 14, 5, 15, 18, 12, 13, 6, 16, 17, 0, 1, 2, 3, 4, 7, 8, 9, 10]
lattice_dirs = [
    (0, 0, 0),
    (1, 0, 0),
    (-1, 0, 0),
    (0, 1, 0),
    (0, -1, 0),
    (0, 0, 1),
    (0, 0, -1),
    (1, 1, 0),
    (-1, -1, 0),
    (1, -1, 0),
    (-1, 1, 0),
    (1, 0, 1),
    (-1, 0, -1),
    (1, 0, -1),
    (-1, 0, 1),
    (0, 1, 1),
    (0, -1, -1),
    (0, 1, -1),
    (0, -1, 1),
]
DIRS = [lattice_dirs[i] for i in ORDER]
FACES = [[p for p in range(19) if DIRS[p][0] == 1], [p for p in range(19) if DIRS[p][0] == -1]]
velocity_scale = 10.0
pair_strength = 0.5
friction = 2.0
time_step = 0.1
MESH = pl.DeviceIdType.MESH


def parts_of(cx):
    edges = list(range(0, cx + 1, 8))
    parts = list(zip(edges[:-1], edges[1:]))
    order = []
    while parts:
        order.append(parts.pop(0))
        if parts:
            order.append(parts.pop())
    return order


def mark(name):
    return contextlib.nullcontext()


def total_of(terms):
    terms = list(terms)
    while len(terms) > 1:
        terms = [a + b for a, b in zip(terms[::2], terms[1::2])] + (
            [terms[-1]] if len(terms) % 2 else []
        )
    return terms[0]


def fields(f):
    density = total_of(f)
    inverse = 1.0 / density
    vel = []
    for axis in range(3):
        plus = total_of(f[p] for p in range(19) if DIRS[p][axis] == 1)
        minus = total_of(f[p] for p in range(19) if DIRS[p][axis] == -1)
        vel.append((plus - minus) * inverse)
    return density, vel


def collided(f, relax):
    density, (vx, vy, vz) = fields(f)
    base = 1.0 - 1.5 * (vx * vx + vy * vy + vz * vz)
    keep = 1.0 - relax
    scale = relax * density
    result = [None] * 19
    for p, c in enumerate(DIRS):
        if result[p] is not None:
            continue
        size = sum(abs(e) for e in c)
        if size == 0:
            result[p] = keep * f[p] + (scale * (1.0 / 3.0)) * base
            continue
        along = total_of(v if e == 1 else -v for e, v in zip(c, (vx, vy, vz)) if e)
        weight = scale * (1.0 / 18.0 if size == 1 else 1.0 / 36.0)
        even = weight * (base + 4.5 * (along * along))
        odd = weight * (3.0 * along)
        q = DIRS.index(tuple(-e for e in c))
        result[p] = keep * f[p] + (even + odd)
        result[q] = keep * f[q] + (even - odd)
    return result


def lane_gather(table, index):
    return jnp.take_along_axis(table, index, axis=1, mode="promise_in_bounds")


def thirds(value):
    parts = []
    for _ in range(3):
        piece = value.astype(jnp.bfloat16).astype(jnp.float32)
        parts.append(piece)
        value = value - piece
    return parts


def by_hits(data, hits, dims):
    return lax.dot_general(
        data.astype(jnp.bfloat16), hits, (dims, ((), ())), preferred_element_type=jnp.float32
    )


def coupled_kernel(
    n_slab,
    n_md,
    f_hbm,
    relax_hbm,
    own_hbm,
    pos_hbm,
    vel_hbm,
    nbr_hbm,
    slots_hbm,
    out_ref,
    pos_out,
    vel_out,
    cell_out,
    f_ref,
    relax_ref,
    own_ref,
    pos_ref,
    vel_ref,
    nbr_ref,
    slots_ref,
    load_sem,
    post,
    rows_out,
    rows_in,
    mean_ref,
    at,
    pull,
    steps_at,
    pairs_at,
    span,
    data,
    hits,
    placed,
    tgt,
    table,
    blocks_out,
    blocks_in,
    send,
    recv,
    swap_send,
    swap_recv,
):
    cz, cx, ny = relax_ref.shape
    top_z = cz - 1
    cells = cz * cx
    entries, atoms = nbr_ref.shape
    groups = atoms // 128
    slot_count = hits.shape[0]
    devices = n_slab * n_md
    cap = slot_count // devices
    parts = parts_of(cx)
    chunks = len(parts)
    outer = [[low for low, _ in parts].index(0), [high for _, high in parts].index(cx)]
    slab, md = lax.axis_index("slab"), lax.axis_index("md")
    me = slab * n_md + md

    def wrapped(value, size):
        return jnp.where(value >= size, value - size, value)

    above, below = wrapped(slab + 1, n_slab), wrapped(slab + n_slab - 1, n_slab)
    right, left = wrapped(md + 1, n_md), wrapped(md + n_md - 1, n_md)
    barrier = pltpu.get_barrier_semaphore()

    def peer_of(k):
        return wrapped(slab + k // n_md, n_slab), wrapped(md + k % n_md, n_md)

    def source_of(k):
        return wrapped(slab + n_slab - k // n_md, n_slab), wrapped(md + n_md - k % n_md, n_md)

    loads = []

    def fetch(src, dst):
        made = pltpu.make_async_copy(src, dst, load_sem.at[len(loads)])
        made.start()
        loads.append(made)
        return made

    f_parts = []
    for low, high in parts[:2] + [(8, cx - 8)]:
        if low < high:
            here = pl.ds(low, high - low)
            f_parts.append(fetch(f_hbm.at[:, :, here, :], f_ref.at[:, :, here, :]))
        if len(f_parts) == 1:
            relax_part = fetch(relax_hbm, relax_ref)
    if max(n_slab // 2, n_md // 2) <= LB_STEPS:
        near = {(a % n_slab) * n_md + b % n_md for a in (-1, 0, 1) for b in (-1, 0, 1)}
        greeted = sorted(near - {0})
    else:
        greeted = list(range(1, devices))
    for k in greeted:
        pl.semaphore_signal(barrier, inc=1, device_id=peer_of(k), device_id_type=MESH)
    pos_parts = [fetch(pos_hbm, pos_ref), fetch(vel_hbm, vel_ref), fetch(nbr_hbm, nbr_ref)]
    slots_part = fetch(slots_hbm, slots_ref)
    own_part = fetch(own_hbm, own_ref)

    def load(step, z, x0):
        if step == 0:
            return [f_ref[ORDER[p], z, pl.ds(x0, 8), :] for p in range(19)]
        return [
            post[step - 1, p, z + 1 - c[2], pl.ds(x0 + (8 - c[0]), 8), :]
            for p, c in enumerate(DIRS)
        ]

    def collide_chunk(step, z, part):
        for x0 in range(*parts[part], 8):
            done = collided(load(step, z, x0), relax_ref[z, pl.ds(x0, 8), :])
            for p, c in enumerate(DIRS):
                value = done[p] if c[1] == 0 else pltpu.roll(done[p], c[1] % ny, axis=1)
                post[step, p, z + 1, pl.ds(x0 + 8, 8), :] = value

    def copy(step, kind, slot, src, dst, peer):
        pltpu.make_async_remote_copy(
            src_ref=src,
            dst_ref=dst,
            send_sem=send.at[kind],
            recv_sem=recv.at[step % 2, slot],
            device_id=peer,
            device_id_type=MESH,
        ).start()

    def whole(src, dst, send_sem, recv_sem):
        return pltpu.make_async_remote_copy(
            src_ref=src,
            dst_ref=dst,
            send_sem=send_sem,
            recv_sem=recv_sem,
            device_id=(above, md),
            device_id_type=MESH,
        )

    arrived = set()

    def arrive(step, slot, ref):
        if (step, slot) in arrived:
            return False
        arrived.add((step, slot))
        whole(ref, ref, send.at[0], recv.at[step % 2, slot]).wait_recv()
        return True

    def save_face(step, z, side):
        row = (7 + cx, 8)[side]
        for j, p in enumerate(FACES[side]):
            rows_out[step, side, z, j, :] = post[step, p, z + 1, row, :]

    def send_face(step, side):
        copy(
            step,
            0,
            side,
            rows_out.at[step, side],
            rows_in.at[step, side, pl.ds(1, cz)],
            (slab, (right, left)[side]),
        )

    def send_edge(step, rising, side):
        z, slot, peer = (top_z, 0, above) if rising else (0, cz + 1, below)
        copy(
            step,
            1,
            side,
            rows_out.at[step, side, z],
            rows_in.at[step, side, slot],
            (peer, (right, left)[side]),
        )

    def send_plane(step, rising, part):
        z, slot, peer = (top_z, 0, above) if rising else (0, cz + 1, below)
        span = pl.ds(0 if rising else 5, 5)
        low, high = parts[part]
        here = pl.ds(8 + low, high - low)
        copy(
            step,
            2,
            2 + part,
            post.at[step, span, z + 1, here, :],
            post.at[step, span, slot, here, :],
            (peer, md),
        )

    def need(step, part):
        for side in range(2):
            if part != outer[side] or not arrive(step, side, rows_in.at[step, side]):
                continue
            row = (7, 8 + cx)[side]
            for j, p in enumerate(FACES[side]):
                for z in range(cz):
                    post[step, p, z + 1, row, :] = rows_in[step, side, z + 1, j, :]
                if DIRS[p][2]:
                    slot = 0 if DIRS[p][2] == 1 else cz + 1
                    post[step, p, slot, row, :] = rows_in[step, side, slot, j, :]
        low, high = parts[part]
        for other, (first, last) in enumerate(parts):
            if first <= high and last >= low:
                here = pl.ds(8 + first, last - first)
                arrive(step, 2 + other, post.at[step, pl.ds(0, 10), 0, here, :])

    def send_chunk(step, rising, part):
        z = top_z if rising else 0
        for side in range(2):
            if part == outer[1 - side]:
                save_face(step, z, side)
                send_edge(step, rising, side)
        send_plane(step, rising, part)

    def lattice_step(step):
        for part in range(chunks):
            if step == 0:
                if part < len(f_parts):
                    f_parts[part].wait()
                if part == 0:
                    relax_part.wait()
            if step:
                with mark("need"):
                    need(step - 1, part)
            for rising in (True, False):
                with mark("collide"):
                    collide_chunk(step, top_z if rising else 0, part)
                if step or part:
                    send_chunk(step, rising, part)
            for z in range(1, top_z):
                collide_chunk(step, z, part)
                for side in range(2):
                    if part == outer[1 - side]:
                        save_face(step, z, side)
            if step == 0 and part == 0:
                with mark("barrier"):
                    pl.semaphore_wait(barrier, len(greeted))
                for rising in (True, False):
                    send_chunk(step, rising, part)
            for side in range(2):
                if part == outer[1 - side]:
                    send_face(step, side)

    def pair_forces():
        for g in range(groups):
            mine = [jnp.broadcast_to(at[c, pl.ds(g, 1), :], (8, 128)) for c in range(3)]
            sums = [jnp.zeros((8, 128), jnp.float32)] * 3
            for k in range(0, entries, 8):
                index = nbr_ref[pl.ds(k, 8), pl.ds(g * 128, 128)]
                lane, row = index & 127, index >> 7
                found = [None] * 3
                for h in range(groups):
                    pick = row == h
                    for c in range(3):
                        line = jnp.broadcast_to(at[c, pl.ds(h, 1), :], (8, 128))
                        value = lane_gather(line, lane)
                        found[c] = value if h == 0 else jnp.where(pick, value, found[c])
                gap = [found[c] - mine[c] for c in range(3)]
                weight = jnp.exp(-0.5 * (gap[0] * gap[0] + gap[1] * gap[1] + gap[2] * gap[2]))
                sums = [sums[c] + gap[c] * weight for c in range(3)]
            for c in range(3):
                pull[c, pl.ds(g, 1), :] = jnp.sum(sums[c], axis=0, keepdims=True)

    half = groups // 2
    levels = 65535.0
    most_pull = 0.6066

    def extreme(value, pick):
        return jnp.broadcast_to(pick(pick(value, axis=0, keepdims=True), axis=1, keepdims=True), (1, 128))

    def prepare_span():
        places = jnp.concatenate([at[c] for c in range(3)], axis=0)
        speeds = jnp.concatenate([at[3 + c] for c in range(3)], axis=0)
        span[pl.ds(0, 1), :] = extreme(places, jnp.min)
        span[pl.ds(1, 1), :] = extreme(places, jnp.max)
        span[pl.ds(2, 1), :] = extreme(jnp.abs(speeds), jnp.max)

    def bound_span(goal, rate):
        far = extreme(jnp.maximum(jnp.maximum(jnp.abs(goal[0]), jnp.abs(goal[1])), jnp.abs(goal[2])), jnp.max)
        least, most = extreme(rate, jnp.min), extreme(rate, jnp.max)
        tame = (least >= 0.0) & (time_step * most <= 1.0)
        strong = time_step * jnp.maximum(jnp.abs(least), jnp.abs(most))
        low, high, speed = (span[pl.ds(i, 1), :] for i in range(3))
        for step in range(1, MD_STEPS):
            speed = jnp.where(tame, jnp.maximum(speed, far), speed + strong * (speed + far))
            speed = (speed + time_step * pair_strength * entries * most_pull) * 1.0001
            low, high = low - time_step * speed, high + time_step * speed
            width = jnp.maximum(high - low, 1e-20)
            span[pl.ds(4 + 2 * step, 1), :] = low
            span[pl.ds(5 + 2 * step, 1), :] = width * (1.0 / levels)

    def coarse_forces(step):
        low = span[pl.ds(4 + 2 * step, 1), :]
        unit = span[pl.ds(5 + 2 * step, 1), :]
        per_unit = 1.0 / unit
        for c in range(3):
            level = jnp.clip((at[c] - low) * per_unit + 0.5, 0.0, levels).astype(jnp.int32)
            steps_at[c] = level
            pairs_at[c] = level[:half] | (level[half:] << 16)
        decay = (-0.5 * 1.4426950408889634) * (unit * unit)
        for g in range(groups):
            mine = [
                jnp.broadcast_to(steps_at[c, pl.ds(g, 1), :].astype(jnp.float32), (8, 128)) for c in range(3)
            ]
            sums = [jnp.zeros((8, 128), jnp.float32)] * 3
            for k in range(0, entries, 8):
                index = nbr_ref[pl.ds(k, 8), pl.ds(g * 128, 128)]
                lane, row = index & 127, index >> 7
                upper = row >= half
                row = jnp.where(upper, row - half, row)
                shift = jnp.where(upper, 16, 0)
                found = [None] * 3
                for h in range(half):
                    pick = row == h
                    for c in range(3):
                        line = jnp.broadcast_to(pairs_at[c, pl.ds(h, 1), :], (8, 128))
                        value = lane_gather(line, lane)
                        found[c] = value if h == 0 else jnp.where(pick, value, found[c])
                gap = [
                    (lax.shift_right_logical(found[c], shift) & 65535).astype(jnp.float32) - mine[c]
                    for c in range(3)
                ]
                weight = jnp.exp2((gap[0] * gap[0] + gap[1] * gap[1] + gap[2] * gap[2]) * decay)
                sums = [sums[c] + gap[c] * weight for c in range(3)]
            for c in range(3):
                pull[c, pl.ds(g, 1), :] = jnp.sum(sums[c], axis=0, keepdims=True) * unit

    def prepare_particles():
        for part in pos_parts:
            part.wait()
        for g in range(groups):
            here = pl.ds(g * 128, 128)
            for c in range(3):
                at[c, pl.ds(g, 1), :] = pos_ref[pl.ds(c, 1), here]
                at[3 + c, pl.ds(g, 1), :] = vel_ref[pl.ds(c, 1), here]
        prepare_span()
        pair_forces()

    def prepare_hits():
        slots_part.wait()
        data[...] = jnp.ones(data.shape, jnp.float32)
        tgt[...] = jnp.zeros(tgt.shape, jnp.float32)
        table[...] = jnp.zeros(table.shape, jnp.float32)
        for g in range(groups):
            label = lax.broadcasted_iota(jnp.int32, (slot_count, 128), 0)
            same = label == slots_ref[pl.ds(g, 1), :]
            hits[:, pl.ds(g * 128, 128)] = jnp.where(same, 1.0, 0.0).astype(jnp.bfloat16)

    def prepare_routes():
        own_part.wait()
        top = own_ref.shape[1]
        owner = [
            jnp.concatenate([own_ref[z, pl.ds(k, 1), :] for z in range(cz)], axis=1)
            for k in range(top)
        ]
        label = lax.broadcasted_iota(jnp.int32, (devices, cells), 0)
        owned = [jnp.where(label == owner[k], 1.0, 0.0) for k in range(top)]
        earlier = lax.broadcasted_iota(jnp.int32, (cells, cells), 0) < lax.broadcasted_iota(
            jnp.int32, (cells, cells), 1
        )
        before = by_hits(
            total_of(owned), jnp.where(earlier, 1.0, 0.0).astype(jnp.bfloat16), ((1,), (0,))
        )
        start = (label * cap).astype(jnp.float32)
        place = lax.broadcasted_iota(jnp.int32, (slot_count, cells), 0).astype(jnp.float32)
        filled = jnp.zeros((slot_count, cells), jnp.float32)
        for k in range(top):
            spot = jnp.sum((before + start) * owned[k], axis=0, keepdims=True)
            filled = filled + jnp.where(place == spot, 1.0, 0.0)
            before = before + owned[k]
        placed[...] = filled.astype(jnp.bfloat16)

    def swap(turn, values, meanwhile):
        per = 128 // cap
        zone = lax.broadcasted_iota(jnp.int32, (4, 128), 1) // cap
        step = lax.broadcasted_iota(jnp.int32, (4, 128), 0)
        for h in range(slot_count // 128):
            turned = pltpu.roll(
                values[:, h * 128 : (h + 1) * 128], 0, axis=1, stride=cap, stride_axis=0
            )
            for j in range(per):
                own = zone == (step + j) % per
                blocks_out[turn, h * per + j] = jnp.sum(
                    jnp.where(own, turned, 0.0), axis=0, keepdims=True
                )
        with mark("begin"):
            for k in sorted(range(1, devices), key=lambda k: -min(k // n_md, n_slab - k // n_md)):
                peer = peer_of(k)
                pltpu.make_async_remote_copy(
                    src_ref=blocks_out.at[turn, peer[0] * n_md + peer[1]],
                    dst_ref=blocks_in.at[turn, me],
                    send_sem=swap_send.at[turn],
                    recv_sem=swap_recv.at[turn],
                    device_id=peer,
                    device_id_type=MESH,
                ).start()
        blocks_in[turn, me] = blocks_out[turn, me]
        meanwhile()
        others = pl.ds(1, devices - 1)
        everyone = whole(
            blocks_out.at[turn, others],
            blocks_in.at[turn, others],
            swap_send.at[turn],
            swap_recv.at[turn],
        )
        with mark("landed"):
            everyone.wait_recv()
        back = 128 - (me % per) * cap
        zone = lax.broadcasted_iota(jnp.int32, (8, 128), 1) // cap
        step = lax.broadcasted_iota(jnp.int32, (8, 128), 0)
        lines = []
        for h in range(slot_count // 128):
            rows = [jnp.zeros((1, 128), jnp.float32)] * 4
            for b in range(per // 8):
                block = pltpu.roll(blocks_in[turn, pl.ds(h * per + b * 8, 8), 0, :], back, axis=1)
                turned = pltpu.roll(block, 0, axis=1, stride=cap, stride_axis=0)
                for c in range(4):
                    row = jnp.sum(
                        jnp.where(zone == (step + c) % per, turned, 0.0), axis=0, keepdims=True
                    )
                    shift = (b * 8 - c) * cap % 128
                    rows[c] = rows[c] + (row if shift == 0 else pltpu.roll(row, shift, axis=1))
            lines.append(jnp.concatenate(rows, axis=0))
        return lines, everyone.wait_send

    lattice_step(0)
    with mark("prep_part"):
        prepare_particles()
    lattice_step(1)
    with mark("hits"):
        prepare_hits()
    lattice_step(2)
    with mark("routes"):
        prepare_routes()
    for step in range(3, LB_STEPS):
        lattice_step(step)

    def finish_chunk(z, part):
        for x0 in range(*parts[part], 8):
            f = load(LB_STEPS, z, x0)
            for p in range(19):
                out_ref[ORDER[p], z, pl.ds(x0, 8), :] = f[p]
            density, vel = fields(f)
            for c, value in enumerate((*vel, density)):
                mean_ref[c, pl.ds(x0 + z * cx, 8), :] = value

    for part in range(chunks):
        with mark("need_last"):
            need(LB_STEPS - 1, part)
        for rising in (True, False):
            finish_chunk(top_z if rising else 0, part)
        for z in range(1, top_z):
            finish_chunk(z, part)

    with mark("mean"):
        for c in range(4):
            scale = (velocity_scale if c < 3 else 1.0) / ny
            mean = jnp.sum(mean_ref[c].T, axis=0, keepdims=True) * scale
            for part, piece in enumerate(thirds(mean)):
                tgt[pl.ds(part * 4 + c, 1), :] = piece
        sums = by_hits(tgt[...], placed[...], ((1,), (1,)))

    def lattice_sent():
        planes = post.at[:, pl.ds(0, 10), 0, pl.ds(8, cx), :]
        for kind, ref in enumerate((rows_out, rows_out.at[:, :, pl.ds(0, 2)], planes)):
            whole(ref, ref, send.at[kind], recv.at[0, 0]).wait_send()

    with mark("swap0"):
        lines, sent_first = swap(0, sums[0:4] + sums[4:8] + sums[8:12], lattice_sent)

    slots = slots_ref[...]
    lane, row = slots & 127, slots >> 7
    goal = []
    for c in range(4):
        value = jnp.zeros((groups, 128), jnp.float32)
        for h, line in enumerate(lines):
            spread = jnp.broadcast_to(line[c : c + 1, :], (groups, 128))
            value = jnp.where(row == h, lane_gather(spread, lane), value)
        goal.append(value)
    rate = friction * goal[3]

    def advance():
        for c in range(3):
            vel = at[3 + c]
            force = pair_strength * pull[c] + rate * (goal[c] - vel)
            vel = vel + time_step * force
            at[3 + c] = vel
            at[c] = at[c] + time_step * vel

    def one_step(step, carry):
        with mark("pair"):
            coarse_forces(step)
        with mark("advance"):
            advance()
        return carry

    bound_span(goal, rate)
    advance()
    lax.fori_loop(1, MD_STEPS, one_step, 0)
    with mark("moments"):
        at[6] = at[3] * at[3] + at[4] * at[4] + at[5] * at[5]
        for c in range(4):
            for part, piece in enumerate(thirds(at[3 + c])):
                for g in range(groups):
                    data[pl.ds(part * 4 + c, 1), pl.ds(g * 128, 128)] = piece[g : g + 1, :]
        sums = by_hits(data[...], hits[...], ((1,), (1,)))
        moments = (sums[0:4] + sums[4:8] + sums[8:12]) / jnp.maximum(sums[12:13], 1.0)

    def put_particles():
        sent_first()
        for g in range(groups):
            here = pl.ds(g * 128, 128)
            for c in range(3):
                pos_out[pl.ds(c, 1), here] = at[c, pl.ds(g, 1), :]
                vel_out[pl.ds(c, 1), here] = at[3 + c, pl.ds(g, 1), :]

    with mark("swap1"):
        lines, sent_second = swap(1, moments, put_particles)
    for h, line in enumerate(lines):
        for part, piece in enumerate(thirds(line)):
            table[pl.ds(part * 4, 4), pl.ds(h * 128, 128)] = piece
    sums = by_hits(table[...], placed[...], ((1,), (0,)))
    picked = sums[0:4] + sums[4:8] + sums[8:12]
    for c in range(4):
        for z in range(cz):
            cell_out[c, pl.ds(z, 1), :] = picked[c : c + 1, z * cx : (z + 1) * cx]
    sent_second()


def put_out(*refs):
    count = len(refs) // 2
    copies = [
        pltpu.make_async_copy(refs[i], refs[count + i], refs[-1].at[i]) for i in range(count)
    ]
    for made in copies:
        made.start()
    for made in copies:
        made.wait()


def on_device(populations, relax, owners, positions, velocities, neighbours, atom_slots):
    cz, cx, ny = relax.shape
    n_slab = lax.axis_size("slab")
    n_md = lax.axis_size("md")
    devices = n_slab * n_md
    top = owners.shape[2]
    cap = cz * max(2, 2 * cx * top // devices)
    slots = devices * cap
    atoms, entries = neighbours.shape
    groups = atoms // 128
    cells = cz * cx
    chunks = len(parts_of(cx))
    vmem = pl.BlockSpec(memory_space=pltpu.VMEM)
    hbm = pl.BlockSpec(memory_space=pltpu.HBM)
    dma = pltpu.SemaphoreType.DMA
    held = [populations.shape, positions.shape, velocities.shape, (4, cz, cx)]
    args = (
        populations,
        relax,
        owners.transpose(0, 2, 1),
        positions,
        velocities,
        neighbours.T,
        atom_slots.reshape(groups, 128),
    )
    results = pl.pallas_call(
        functools.partial(coupled_kernel, n_slab, n_md),
        out_shape=tuple(pltpu.VMEM(shape, jnp.float32) for shape in held),
        in_specs=[hbm] * 7,
        out_specs=(vmem,) * 4,
        scratch_shapes=[
            pltpu.VMEM(populations.shape, jnp.float32),
            pltpu.VMEM(relax.shape, jnp.float32),
            pltpu.VMEM((cz, top, cx), jnp.int32),
            pltpu.VMEM(positions.shape, jnp.float32),
            pltpu.VMEM(velocities.shape, jnp.float32),
            pltpu.VMEM((entries, atoms), jnp.int32),
            pltpu.VMEM((groups, 128), jnp.int32),
            dma((9,)),
            pltpu.VMEM((LB_STEPS, 19, cz + 2, cx + 16, ny), jnp.float32),
            pltpu.VMEM((LB_STEPS, 2, cz, 8, ny), jnp.float32),
            pltpu.VMEM((LB_STEPS, 2, cz + 2, 8, ny), jnp.float32),
            pltpu.VMEM((4, cells, ny), jnp.float32),
            pltpu.VMEM((7, groups, 128), jnp.float32),
            pltpu.VMEM((3, groups, 128), jnp.float32),
            pltpu.VMEM((3, groups, 128), jnp.int32),
            pltpu.VMEM((3, groups // 2, 128), jnp.int32),
            pltpu.VMEM((4 + 2 * MD_STEPS, 128), jnp.float32),
            pltpu.VMEM((16, atoms), jnp.float32),
            pltpu.VMEM((slots, atoms), jnp.bfloat16),
            pltpu.VMEM((slots, cells), jnp.bfloat16),
            pltpu.VMEM((16, cells), jnp.float32),
            pltpu.VMEM((16, slots), jnp.float32),
            pltpu.VMEM((2, devices, 1, 128), jnp.float32),
            pltpu.VMEM((2, devices, 1, 128), jnp.float32),
            dma((3,)),
            dma((2, 2 + chunks)),
            dma((2,)),
            dma((2,)),
        ],
        compiler_params=pltpu.CompilerParams(
            collective_id=0, has_side_effects=True, vmem_limit_bytes=48 * 1024 * 1024
        ),
        name="coupled",
    )(*(pltpu.with_memory_space_constraint(arg, pltpu.HBM) for arg in args))
    return pl.pallas_call(
        put_out,
        out_shape=tuple(jax.ShapeDtypeStruct(shape, jnp.float32) for shape in held),
        in_specs=[vmem] * 4,
        out_specs=(hbm,) * 4,
        scratch_shapes=[dma((4,))],
        compiler_params=pltpu.CompilerParams(vmem_limit_bytes=4 * 1024 * 1024),
        name="put_out",
    )(*(pltpu.with_memory_space_constraint(part, pltpu.VMEM) for part in results))


def solution(mesh):
    return jax.shard_map(
        on_device,
        mesh=mesh,
        in_specs=(
            P(None, "slab", "md", None),
            P("slab", "md", None),
            P("slab", "md", None),
            P(None, ("slab", "md")),
            P(None, ("slab", "md")),
            P(("slab", "md"), None),
            P(("slab", "md")),
        ),
        out_specs=(
            P(None, "slab", "md", None),
            P(None, ("slab", "md")),
            P(None, ("slab", "md")),
            P(None, "slab", "md"),
        ),
        check_vma=False,
    )
```

```python
import contextlib
import functools

import jax
import jax.numpy as jnp
from jax import lax
from jax.experimental import pallas as pl
from jax.experimental.pallas import tpu as pltpu
from jax.sharding import PartitionSpec as P

LB_STEPS = 4
MD_STEPS = 5

ORDER = [11, 14, 5, 15, 18, 12, 13, 6, 16, 17, 0, 1, 2, 3, 4, 7, 8, 9, 10]
lattice_dirs = [
    (0, 0, 0),
    (1, 0, 0),
    (-1, 0, 0),
    (0, 1, 0),
    (0, -1, 0),
    (0, 0, 1),
    (0, 0, -1),
    (1, 1, 0),
    (-1, -1, 0),
    (1, -1, 0),
    (-1, 1, 0),
    (1, 0, 1),
    (-1, 0, -1),
    (1, 0, -1),
    (-1, 0, 1),
    (0, 1, 1),
    (0, -1, -1),
    (0, 1, -1),
    (0, -1, 1),
]
DIRS = [lattice_dirs[i] for i in ORDER]
FACES = [[p for p in range(19) if DIRS[p][0] == 1], [p for p in range(19) if DIRS[p][0] == -1]]
velocity_scale = 10.0
pair_strength = 0.5
friction = 2.0
time_step = 0.1
MESH = pl.DeviceIdType.MESH


def parts_of(cx):
    edges = list(range(0, cx + 1, 8))
    parts = list(zip(edges[:-1], edges[1:]))
    order = []
    while parts:
        order.append(parts.pop(0))
        if parts:
            order.append(parts.pop())
    return order


def mark(name):
    return contextlib.nullcontext()


def total_of(terms):
    terms = list(terms)
    while len(terms) > 1:
        terms = [a + b for a, b in zip(terms[::2], terms[1::2])] + (
            [terms[-1]] if len(terms) % 2 else []
        )
    return terms[0]


def fields(f):
    density = total_of(f)
    inverse = 1.0 / density
    vel = []
    for axis in range(3):
        plus = total_of(f[p] for p in range(19) if DIRS[p][axis] == 1)
        minus = total_of(f[p] for p in range(19) if DIRS[p][axis] == -1)
        vel.append((plus - minus) * inverse)
    return density, vel


def collided(f, relax):
    density, (vx, vy, vz) = fields(f)
    base = 1.0 - 1.5 * (vx * vx + vy * vy + vz * vz)
    keep = 1.0 - relax
    scale = relax * density
    result = [None] * 19
    for p, c in enumerate(DIRS):
        if result[p] is not None:
            continue
        size = sum(abs(e) for e in c)
        if size == 0:
            result[p] = keep * f[p] + (scale * (1.0 / 3.0)) * base
            continue
        along = total_of(v if e == 1 else -v for e, v in zip(c, (vx, vy, vz)) if e)
        weight = scale * (1.0 / 18.0 if size == 1 else 1.0 / 36.0)
        even = weight * (base + 4.5 * (along * along))
        odd = weight * (3.0 * along)
        q = DIRS.index(tuple(-e for e in c))
        result[p] = keep * f[p] + (even + odd)
        result[q] = keep * f[q] + (even - odd)
    return result


def lane_gather(table, index):
    return jnp.take_along_axis(table, index, axis=1, mode="promise_in_bounds")


def thirds(value):
    parts = []
    for _ in range(3):
        piece = value.astype(jnp.bfloat16).astype(jnp.float32)
        parts.append(piece)
        value = value - piece
    return parts


def by_hits(data, hits, dims):
    return lax.dot_general(
        data.astype(jnp.bfloat16), hits, (dims, ((), ())), preferred_element_type=jnp.float32
    )


def coupled_kernel(
    n_slab,
    n_md,
    f_hbm,
    relax_hbm,
    own_hbm,
    pos_hbm,
    vel_hbm,
    nbr_hbm,
    slots_hbm,
    out_ref,
    pos_out,
    vel_out,
    cell_out,
    f_ref,
    relax_ref,
    own_ref,
    pos_ref,
    vel_ref,
    nbr_ref,
    slots_ref,
    load_sem,
    post,
    rows_out,
    rows_in,
    edge_out,
    edge_in,
    mean_ref,
    at,
    pull,
    steps_at,
    pairs_at,
    span,
    data,
    hits,
    placed,
    tgt,
    table,
    blocks_out,
    blocks_in,
    send,
    recv,
    swap_send,
    swap_recv,
):
    cz, cx, ny = relax_ref.shape
    top_z = cz - 1
    cells = cz * cx
    entries, atoms = nbr_ref.shape
    groups = atoms // 128
    slot_count = hits.shape[0]
    devices = n_slab * n_md
    cap = slot_count // devices
    parts = parts_of(cx)
    chunks = len(parts)
    outer = [[low for low, _ in parts].index(0), [high for _, high in parts].index(cx)]
    slab, md = lax.axis_index("slab"), lax.axis_index("md")
    me = slab * n_md + md

    def wrapped(value, size):
        return jnp.where(value >= size, value - size, value)

    above, below = wrapped(slab + 1, n_slab), wrapped(slab + n_slab - 1, n_slab)
    right, left = wrapped(md + 1, n_md), wrapped(md + n_md - 1, n_md)
    barrier = pltpu.get_barrier_semaphore()

    def peer_of(k):
        return wrapped(slab + k // n_md, n_slab), wrapped(md + k % n_md, n_md)

    def source_of(k):
        return wrapped(slab + n_slab - k // n_md, n_slab), wrapped(md + n_md - k % n_md, n_md)

    loads = []

    def fetch(src, dst):
        made = pltpu.make_async_copy(src, dst, load_sem.at[len(loads)])
        made.start()
        loads.append(made)
        return made

    f_parts = []
    for low, high in parts[:2] + [(8, cx - 8)]:
        if low < high:
            here = pl.ds(low, high - low)
            f_parts.append(fetch(f_hbm.at[:, :, here, :], f_ref.at[:, :, here, :]))
        if len(f_parts) == 1:
            relax_part = fetch(relax_hbm, relax_ref)
    if max(n_slab // 2, n_md // 2) <= LB_STEPS:
        near = {(a % n_slab) * n_md + b % n_md for a in (-1, 0, 1) for b in (-1, 0, 1)}
        greeted = sorted(near - {0})
    else:
        greeted = list(range(1, devices))
    for k in greeted:
        pl.semaphore_signal(barrier, inc=1, device_id=peer_of(k), device_id_type=MESH)
    pos_parts = [fetch(pos_hbm, pos_ref), fetch(vel_hbm, vel_ref), fetch(nbr_hbm, nbr_ref)]
    slots_part = fetch(slots_hbm, slots_ref)
    own_part = fetch(own_hbm, own_ref)

    def load(step, z, x0):
        if step == 0:
            return [f_ref[ORDER[p], z, pl.ds(x0, 8), :] for p in range(19)]
        return [
            post[step - 1, p, z + 1 - c[2], pl.ds(x0 + (8 - c[0]), 8), :]
            for p, c in enumerate(DIRS)
        ]

    def collide_chunk(step, z, part):
        for x0 in range(*parts[part], 8):
            done = collided(load(step, z, x0), relax_ref[z, pl.ds(x0, 8), :])
            for p, c in enumerate(DIRS):
                value = done[p] if c[1] == 0 else pltpu.roll(done[p], c[1] % ny, axis=1)
                post[step, p, z + 1, pl.ds(x0 + 8, 8), :] = value

    def copy(step, kind, slot, src, dst, peer):
        pltpu.make_async_remote_copy(
            src_ref=src,
            dst_ref=dst,
            send_sem=send.at[kind],
            recv_sem=recv.at[step % 2, slot],
            device_id=peer,
            device_id_type=MESH,
        ).start()

    def whole(src, dst, send_sem, recv_sem):
        return pltpu.make_async_remote_copy(
            src_ref=src,
            dst_ref=dst,
            send_sem=send_sem,
            recv_sem=recv_sem,
            device_id=(above, md),
            device_id_type=MESH,
        )

    arrived = set()

    def arrive(step, slot, ref):
        if (step, slot) in arrived:
            return False
        arrived.add((step, slot))
        whole(ref, ref, send.at[0], recv.at[step % 2, slot]).wait_recv()
        return True

    def save_face(step, z, side):
        row = (7 + cx, 8)[side]
        for j, p in enumerate(FACES[side]):
            rows_out[step, side, z, j, :] = post[step, p, z + 1, row, :]

    def send_face(step, side):
        copy(
            step,
            0,
            side,
            rows_out.at[step, side],
            rows_in.at[step, side],
            (slab, (right, left)[side]),
        )

    EDGES = [[DIRS.index((x, 0, z)) for z in (-1, 1)] for x in (1, -1)]

    def send_edge(step, rising, side):
        z, peer = (top_z, above) if rising else (0, below)
        row = (7 + cx, 8)[side]
        edge_out[step, side, int(rising), 0, :] = post[step, EDGES[side][int(rising)], z + 1, row, :]
        copy(
            step,
            1,
            2 + side,
            edge_out.at[step, side, int(rising)],
            edge_in.at[step, side, int(rising)],
            (peer, (right, left)[side]),
        )

    def send_plane(step, rising, part):
        z, slot, peer = (top_z, 0, above) if rising else (0, cz + 1, below)
        span = pl.ds(0 if rising else 5, 5)
        low, high = parts[part]
        here = pl.ds(8 + low, high - low)
        copy(
            step,
            2,
            4 + part,
            post.at[step, span, z + 1, here, :],
            post.at[step, span, slot, here, :],
            (peer, md),
        )

    def need(step, part):
        for side in range(2):
            if part != outer[side] or not arrive(step, side, rows_in.at[step, side]):
                continue
            row = (7, 8 + cx)[side]
            for j, p in enumerate(FACES[side]):
                for z in range(cz):
                    post[step, p, z + 1, row, :] = rows_in[step, side, z, j, :]
            arrive(step, 2 + side, edge_in.at[step, side])
            for rising in range(2):
                slot = 0 if rising else cz + 1
                post[step, EDGES[side][rising], slot, row, :] = edge_in[step, side, rising, 0, :]
        low, high = parts[part]
        for other, (first, last) in enumerate(parts):
            if first <= high and last >= low:
                here = pl.ds(8 + first, last - first)
                arrive(step, 4 + other, post.at[step, pl.ds(0, 10), 0, here, :])

    def send_chunk(step, rising, part):
        z = top_z if rising else 0
        for side in range(2):
            if part == outer[1 - side]:
                save_face(step, z, side)
                send_edge(step, rising, side)
        send_plane(step, rising, part)

    def lattice_step(step):
        for part in range(chunks):
            if step == 0:
                if part < len(f_parts):
                    f_parts[part].wait()
                if part == 0:
                    relax_part.wait()
            if step:
                with mark("need"):
                    need(step - 1, part)
            for rising in (True, False):
                with mark("collide"):
                    collide_chunk(step, top_z if rising else 0, part)
                if step or part:
                    send_chunk(step, rising, part)
            for z in range(1, top_z):
                collide_chunk(step, z, part)
                for side in range(2):
                    if part == outer[1 - side]:
                        save_face(step, z, side)
            if step == 0 and part == 0:
                with mark("barrier"):
                    pl.semaphore_wait(barrier, len(greeted))
                for rising in (True, False):
                    send_chunk(step, rising, part)
            for side in range(2):
                if part == outer[1 - side]:
                    send_face(step, side)

    def pair_forces():
        for g in range(groups):
            mine = [jnp.broadcast_to(at[c, pl.ds(g, 1), :], (8, 128)) for c in range(3)]
            sums = [jnp.zeros((8, 128), jnp.float32)] * 3
            for k in range(0, entries, 8):
                index = nbr_ref[pl.ds(k, 8), pl.ds(g * 128, 128)]
                lane, row = index & 127, index >> 7
                found = [None] * 3
                for h in range(groups):
                    pick = row == h
                    for c in range(3):
                        line = jnp.broadcast_to(at[c, pl.ds(h, 1), :], (8, 128))
                        value = lane_gather(line, lane)
                        found[c] = value if h == 0 else jnp.where(pick, value, found[c])
                gap = [found[c] - mine[c] for c in range(3)]
                weight = jnp.exp(-0.5 * (gap[0] * gap[0] + gap[1] * gap[1] + gap[2] * gap[2]))
                sums = [sums[c] + gap[c] * weight for c in range(3)]
            for c in range(3):
                pull[c, pl.ds(g, 1), :] = jnp.sum(sums[c], axis=0, keepdims=True)

    half = groups // 2
    levels = 65535.0
    most_pull = 0.6066

    def extreme(value, pick):
        return jnp.broadcast_to(pick(pick(value, axis=0, keepdims=True), axis=1, keepdims=True), (1, 128))

    def prepare_span():
        places = jnp.concatenate([at[c] for c in range(3)], axis=0)
        speeds = jnp.concatenate([at[3 + c] for c in range(3)], axis=0)
        span[pl.ds(0, 1), :] = extreme(places, jnp.min)
        span[pl.ds(1, 1), :] = extreme(places, jnp.max)
        span[pl.ds(2, 1), :] = extreme(jnp.abs(speeds), jnp.max)

    def bound_span(blocks):
        per = 128 // cap
        zone = lax.broadcasted_iota(jnp.int32, (8, 128), 1) // cap
        last = zone == lax.rem(lax.rem(me, per) + 3, per)
        largest = smallest = None
        strength = jnp.zeros((8, 128), jnp.float32)
        for block in blocks:
            strength = jnp.maximum(strength, jnp.where(last, 0.0, jnp.abs(block)))
            rate = jnp.where(last, friction * block, 0.0)
            largest = rate if largest is None else jnp.maximum(largest, rate)
            smallest = rate if smallest is None else jnp.minimum(smallest, rate)
        far, least, most = extreme(strength, jnp.max), extreme(smallest, jnp.min), extreme(largest, jnp.max)
        tame = (least >= 0.0) & (time_step * most <= 1.0)
        strong = time_step * jnp.maximum(jnp.abs(least), jnp.abs(most))
        low, high, speed = (span[pl.ds(i, 1), :] for i in range(3))
        for step in range(1, MD_STEPS):
            speed = jnp.where(tame, jnp.maximum(speed, far), speed + strong * (speed + far))
            speed = (speed + time_step * pair_strength * entries * most_pull) * 1.0001
            low, high = low - time_step * speed, high + time_step * speed
            width = jnp.maximum(high - low, 1e-20)
            span[pl.ds(4 + 2 * step, 1), :] = low
            span[pl.ds(5 + 2 * step, 1), :] = width * (1.0 / levels)

    def coarse_forces(step):
        low = span[pl.ds(4 + 2 * step, 1), :]
        unit = span[pl.ds(5 + 2 * step, 1), :]
        per_unit = 1.0 / unit
        for c in range(3):
            level = jnp.clip((at[c] - low) * per_unit + 0.5, 0.0, levels).astype(jnp.int32)
            steps_at[c] = level
            pairs_at[c] = level[:half] | (level[half:] << 16)
        decay = (-0.5 * 1.4426950408889634) * (unit * unit)
        for g in range(groups):
            mine = [
                jnp.broadcast_to(steps_at[c, pl.ds(g, 1), :].astype(jnp.float32), (8, 128)) for c in range(3)
            ]
            sums = [jnp.zeros((8, 128), jnp.float32)] * 3
            for k in range(0, entries, 8):
                index = nbr_ref[pl.ds(k, 8), pl.ds(g * 128, 128)]
                lane, row = index & 127, index >> 7
                upper = row >= half
                row = jnp.where(upper, row - half, row)
                shift = jnp.where(upper, 16, 0)
                found = [None] * 3
                for h in range(half):
                    pick = row == h
                    for c in range(3):
                        line = jnp.broadcast_to(pairs_at[c, pl.ds(h, 1), :], (8, 128))
                        value = lane_gather(line, lane)
                        found[c] = value if h == 0 else jnp.where(pick, value, found[c])
                gap = [
                    (lax.shift_right_logical(found[c], shift) & 65535).astype(jnp.float32) - mine[c]
                    for c in range(3)
                ]
                weight = jnp.exp2((gap[0] * gap[0] + gap[1] * gap[1] + gap[2] * gap[2]) * decay)
                sums = [sums[c] + gap[c] * weight for c in range(3)]
            for c in range(3):
                pull[c, pl.ds(g, 1), :] = jnp.sum(sums[c], axis=0, keepdims=True) * unit

    def prepare_particles():
        for part in pos_parts:
            part.wait()
        for g in range(groups):
            here = pl.ds(g * 128, 128)
            for c in range(3):
                at[c, pl.ds(g, 1), :] = pos_ref[pl.ds(c, 1), here]
                at[3 + c, pl.ds(g, 1), :] = vel_ref[pl.ds(c, 1), here]
        prepare_span()
        pair_forces()

    def prepare_hits():
        slots_part.wait()
        data[...] = jnp.ones(data.shape, jnp.float32)
        tgt[...] = jnp.zeros(tgt.shape, jnp.float32)
        table[...] = jnp.zeros(table.shape, jnp.float32)
        for g in range(groups):
            label = lax.broadcasted_iota(jnp.int32, (slot_count, 128), 0)
            same = label == slots_ref[pl.ds(g, 1), :]
            hits[:, pl.ds(g * 128, 128)] = jnp.where(same, 1.0, 0.0).astype(jnp.bfloat16)

    def prepare_routes():
        own_part.wait()
        top = own_ref.shape[1]
        owner = [
            jnp.concatenate([own_ref[z, pl.ds(k, 1), :] for z in range(cz)], axis=1)
            for k in range(top)
        ]
        label = lax.broadcasted_iota(jnp.int32, (devices, cells), 0)
        owned = [jnp.where(label == owner[k], 1.0, 0.0) for k in range(top)]
        earlier = lax.broadcasted_iota(jnp.int32, (cells, cells), 0) < lax.broadcasted_iota(
            jnp.int32, (cells, cells), 1
        )
        before = by_hits(
            total_of(owned), jnp.where(earlier, 1.0, 0.0).astype(jnp.bfloat16), ((1,), (0,))
        )
        start = (label * cap).astype(jnp.float32)
        place = lax.broadcasted_iota(jnp.int32, (slot_count, cells), 0).astype(jnp.float32)
        filled = jnp.zeros((slot_count, cells), jnp.float32)
        for k in range(top):
            spot = jnp.sum((before + start) * owned[k], axis=0, keepdims=True)
            filled = filled + jnp.where(place == spot, 1.0, 0.0)
            before = before + owned[k]
        placed[...] = filled.astype(jnp.bfloat16)

    def swap(turn, values, meanwhile):
        per = 128 // cap
        zone = lax.broadcasted_iota(jnp.int32, (4, 128), 1) // cap
        step = lax.broadcasted_iota(jnp.int32, (4, 128), 0)
        for h in range(slot_count // 128):
            turned = pltpu.roll(
                values[:, h * 128 : (h + 1) * 128], 0, axis=1, stride=cap, stride_axis=0
            )
            for j in range(per):
                own = zone == (step + j) % per
                blocks_out[turn, h * per + j] = jnp.sum(
                    jnp.where(own, turned, 0.0), axis=0, keepdims=True
                )
        with mark("begin"):
            for k in sorted(range(1, devices), key=lambda k: -min(k // n_md, n_slab - k // n_md)):
                peer = peer_of(k)
                pltpu.make_async_remote_copy(
                    src_ref=blocks_out.at[turn, peer[0] * n_md + peer[1]],
                    dst_ref=blocks_in.at[turn, me],
                    send_sem=swap_send.at[turn],
                    recv_sem=swap_recv.at[turn],
                    device_id=peer,
                    device_id_type=MESH,
                ).start()
        blocks_in[turn, me] = blocks_out[turn, me]
        meanwhile()
        others = pl.ds(1, devices - 1)
        everyone = whole(
            blocks_out.at[turn, others],
            blocks_in.at[turn, others],
            swap_send.at[turn],
            swap_recv.at[turn],
        )
        with mark("landed"):
            everyone.wait_recv()
        place = lax.rem(me, per)
        zone = lax.broadcasted_iota(jnp.int32, (8, 128), 1) // cap
        step = lax.broadcasted_iota(jnp.int32, (8, 128), 0)
        lines, blocks = [], []
        for h in range(slot_count // 128):
            rows = [jnp.zeros((1, 128), jnp.float32)] * 4
            for b in range(per // 8):
                block = blocks_in[turn, pl.ds(h * per + b * 8, 8), 0, :]
                blocks.append(block)
                turned = pltpu.roll(block, 0, axis=1, stride=cap, stride_axis=0)
                for c in range(4):
                    own = zone == lax.rem(step + (c + place), per)
                    row = jnp.sum(jnp.where(own, turned, 0.0), axis=0, keepdims=True)
                    shift = b * 8 * cap
                    rows[c] = rows[c] + (row if shift == 0 else pltpu.roll(row, shift, axis=1))
            lines.append(rows)
        return lines, blocks, everyone.wait_send

    lattice_step(0)
    with mark("prep_part"):
        prepare_particles()
    lattice_step(1)
    with mark("hits"):
        prepare_hits()
    lattice_step(2)
    with mark("routes"):
        prepare_routes()
    for step in range(3, LB_STEPS):
        lattice_step(step)

    def finish_chunk(z, part):
        for x0 in range(*parts[part], 8):
            f = load(LB_STEPS, z, x0)
            for p in range(19):
                out_ref[ORDER[p], z, pl.ds(x0, 8), :] = f[p]
            density, vel = fields(f)
            for c, value in enumerate((*vel, density)):
                mean_ref[c, pl.ds(x0 + z * cx, 8), :] = value

    for part in range(chunks):
        with mark("need_last"):
            need(LB_STEPS - 1, part)
        for rising in (True, False):
            finish_chunk(top_z if rising else 0, part)
        for z in range(1, top_z):
            finish_chunk(z, part)

    with mark("mean"):
        for c in range(4):
            scale = (velocity_scale if c < 3 else 1.0) / ny
            mean = jnp.sum(mean_ref[c].T, axis=0, keepdims=True) * scale
            for part, piece in enumerate(thirds(mean)):
                tgt[pl.ds(part * 4 + c, 1), :] = piece
        sums = by_hits(tgt[...], placed[...], ((1,), (1,)))

    def lattice_sent():
        planes = post.at[:, pl.ds(0, 10), 0, pl.ds(8, cx), :]
        for kind, ref in enumerate((rows_out, edge_out, planes)):
            whole(ref, ref, send.at[kind], recv.at[0, 0]).wait_send()

    with mark("swap0"):
        lines, blocks, sent_first = swap(0, sums[0:4] + sums[4:8] + sums[8:12], lattice_sent)

    per = 128 // cap
    slots = slots_ref[...]
    row = slots >> 7
    goal = []
    for c in range(4):
        lane = (slots + (c + lax.rem(me, per)) * cap) & 127
        value = jnp.zeros((groups, 128), jnp.float32)
        for h, line in enumerate(lines):
            spread = jnp.broadcast_to(line[c], (groups, 128))
            value = jnp.where(row == h, lane_gather(spread, lane), value)
        goal.append(value)
    rate = friction * goal[3]

    def advance():
        for c in range(3):
            vel = at[3 + c]
            force = pair_strength * pull[c] + rate * (goal[c] - vel)
            vel = vel + time_step * force
            at[3 + c] = vel
            at[c] = at[c] + time_step * vel

    def one_step(step, carry):
        with mark("pair"):
            coarse_forces(step)
        with mark("advance"):
            advance()
        return carry

    bound_span(blocks)
    advance()
    lax.fori_loop(1, MD_STEPS, one_step, 0)
    with mark("moments"):
        at[6] = at[3] * at[3] + at[4] * at[4] + at[5] * at[5]
        for c in range(4):
            for part, piece in enumerate(thirds(at[3 + c])):
                for g in range(groups):
                    data[pl.ds(part * 4 + c, 1), pl.ds(g * 128, 128)] = piece[g : g + 1, :]
        sums = by_hits(data[...], hits[...], ((1,), (1,)))
        moments = (sums[0:4] + sums[4:8] + sums[8:12]) / jnp.maximum(sums[12:13], 1.0)

    def put_particles():
        sent_first()
        for g in range(groups):
            here = pl.ds(g * 128, 128)
            for c in range(3):
                pos_out[pl.ds(c, 1), here] = at[c, pl.ds(g, 1), :]
                vel_out[pl.ds(c, 1), here] = at[3 + c, pl.ds(g, 1), :]

    with mark("swap1"):
        lines, _, sent_second = swap(1, moments, put_particles)
    for h, line in enumerate(lines):
        for c in range(4):
            whole_line = pltpu.roll(line[c], 128 - lax.rem(c + lax.rem(me, per), per) * cap, axis=1)
            for part, piece in enumerate(thirds(whole_line)):
                table[pl.ds(part * 4 + c, 1), pl.ds(h * 128, 128)] = piece
    sums = by_hits(table[...], placed[...], ((1,), (0,)))
    picked = sums[0:4] + sums[4:8] + sums[8:12]
    for c in range(4):
        for z in range(cz):
            cell_out[c, pl.ds(z, 1), :] = picked[c : c + 1, z * cx : (z + 1) * cx]
    sent_second()


def put_out(*refs):
    count = len(refs) // 2
    copies = [
        pltpu.make_async_copy(refs[i], refs[count + i], refs[-1].at[i]) for i in range(count)
    ]
    for made in copies:
        made.start()
    for made in copies:
        made.wait()


def on_device(populations, relax, owners, positions, velocities, neighbours, atom_slots):
    cz, cx, ny = relax.shape
    n_slab = lax.axis_size("slab")
    n_md = lax.axis_size("md")
    devices = n_slab * n_md
    top = owners.shape[2]
    cap = cz * max(2, 2 * cx * top // devices)
    slots = devices * cap
    atoms, entries = neighbours.shape
    groups = atoms // 128
    cells = cz * cx
    chunks = len(parts_of(cx))
    vmem = pl.BlockSpec(memory_space=pltpu.VMEM)
    hbm = pl.BlockSpec(memory_space=pltpu.HBM)
    dma = pltpu.SemaphoreType.DMA
    held = [populations.shape, positions.shape, velocities.shape, (4, cz, cx)]
    args = (
        populations,
        relax,
        owners.transpose(0, 2, 1),
        positions,
        velocities,
        neighbours.T,
        atom_slots.reshape(groups, 128),
    )
    results = pl.pallas_call(
        functools.partial(coupled_kernel, n_slab, n_md),
        out_shape=tuple(pltpu.VMEM(shape, jnp.float32) for shape in held),
        in_specs=[hbm] * 7,
        out_specs=(vmem,) * 4,
        scratch_shapes=[
            pltpu.VMEM(populations.shape, jnp.float32),
            pltpu.VMEM(relax.shape, jnp.float32),
            pltpu.VMEM((cz, top, cx), jnp.int32),
            pltpu.VMEM(positions.shape, jnp.float32),
            pltpu.VMEM(velocities.shape, jnp.float32),
            pltpu.VMEM((entries, atoms), jnp.int32),
            pltpu.VMEM((groups, 128), jnp.int32),
            dma((9,)),
            pltpu.VMEM((LB_STEPS, 19, cz + 2, cx + 16, ny), jnp.float32),
            pltpu.VMEM((LB_STEPS, 2, cz, 8, ny), jnp.float32),
            pltpu.VMEM((LB_STEPS, 2, cz, 8, ny), jnp.float32),
            pltpu.VMEM((LB_STEPS, 2, 2, 1, ny), jnp.float32),
            pltpu.VMEM((LB_STEPS, 2, 2, 1, ny), jnp.float32),
            pltpu.VMEM((4, cells, ny), jnp.float32),
            pltpu.VMEM((7, groups, 128), jnp.float32),
            pltpu.VMEM((3, groups, 128), jnp.float32),
            pltpu.VMEM((3, groups, 128), jnp.int32),
            pltpu.VMEM((3, groups // 2, 128), jnp.int32),
            pltpu.VMEM((4 + 2 * MD_STEPS, 128), jnp.float32),
            pltpu.VMEM((16, atoms), jnp.float32),
            pltpu.VMEM((slots, atoms), jnp.bfloat16),
            pltpu.VMEM((slots, cells), jnp.bfloat16),
            pltpu.VMEM((16, cells), jnp.float32),
            pltpu.VMEM((16, slots), jnp.float32),
            pltpu.VMEM((2, devices, 1, 128), jnp.float32),
            pltpu.VMEM((2, devices, 1, 128), jnp.float32),
            dma((3,)),
            dma((2, 4 + chunks)),
            dma((2,)),
            dma((2,)),
        ],
        compiler_params=pltpu.CompilerParams(
            collective_id=0, has_side_effects=True, vmem_limit_bytes=48 * 1024 * 1024
        ),
        name="coupled",
    )(*(pltpu.with_memory_space_constraint(arg, pltpu.HBM) for arg in args))
    return pl.pallas_call(
        put_out,
        out_shape=tuple(jax.ShapeDtypeStruct(shape, jnp.float32) for shape in held),
        in_specs=[vmem] * 4,
        out_specs=(hbm,) * 4,
        scratch_shapes=[dma((4,))],
        compiler_params=pltpu.CompilerParams(vmem_limit_bytes=4 * 1024 * 1024),
        name="put_out",
    )(*(pltpu.with_memory_space_constraint(part, pltpu.VMEM) for part in results))


def solution(mesh):
    return jax.shard_map(
        on_device,
        mesh=mesh,
        in_specs=(
            P(None, "slab", "md", None),
            P("slab", "md", None),
            P("slab", "md", None),
            P(None, ("slab", "md")),
            P(None, ("slab", "md")),
            P(("slab", "md"), None),
            P(("slab", "md")),
        ),
        out_specs=(
            P(None, "slab", "md", None),
            P(None, ("slab", "md")),
            P(None, ("slab", "md")),
            P(None, "slab", "md"),
        ),
        check_vma=False,
    )
```

```python
import contextlib
import functools

import jax
import jax.numpy as jnp
from jax import lax
from jax.experimental import pallas as pl
from jax.experimental.pallas import tpu as pltpu
from jax.sharding import PartitionSpec as P

LB_STEPS = 4
MD_STEPS = 5

ORDER = [11, 14, 5, 15, 18, 12, 13, 6, 16, 17, 0, 1, 2, 3, 4, 7, 8, 9, 10]
lattice_dirs = [
    (0, 0, 0),
    (1, 0, 0),
    (-1, 0, 0),
    (0, 1, 0),
    (0, -1, 0),
    (0, 0, 1),
    (0, 0, -1),
    (1, 1, 0),
    (-1, -1, 0),
    (1, -1, 0),
    (-1, 1, 0),
    (1, 0, 1),
    (-1, 0, -1),
    (1, 0, -1),
    (-1, 0, 1),
    (0, 1, 1),
    (0, -1, -1),
    (0, 1, -1),
    (0, -1, 1),
]
DIRS = [lattice_dirs[i] for i in ORDER]
FACES = [[p for p in range(19) if DIRS[p][0] == 1], [p for p in range(19) if DIRS[p][0] == -1]]
STEEP = [[DIRS.index((0, y, z)) for y in (0, 1, -1)] for z in (1, -1)]
velocity_scale = 10.0
pair_strength = 0.5
friction = 2.0
time_step = 0.1
MESH = pl.DeviceIdType.MESH


def parts_of(cx):
    edges = list(range(0, cx + 1, 8))
    parts = list(zip(edges[:-1], edges[1:]))
    order = []
    while parts:
        order.append(parts.pop(0))
        if parts:
            order.append(parts.pop())
    return order


def mark(name):
    return contextlib.nullcontext()


def total_of(terms):
    terms = list(terms)
    while len(terms) > 1:
        terms = [a + b for a, b in zip(terms[::2], terms[1::2])] + (
            [terms[-1]] if len(terms) % 2 else []
        )
    return terms[0]


def fields(f):
    density = total_of(f)
    inverse = 1.0 / density
    vel = []
    for axis in range(3):
        plus = total_of(f[p] for p in range(19) if DIRS[p][axis] == 1)
        minus = total_of(f[p] for p in range(19) if DIRS[p][axis] == -1)
        vel.append((plus - minus) * inverse)
    return density, vel


def merged_fields(f, merged):
    steep = [p for side in merged for p in STEEP[side]]
    rest = [p for p in range(19) if p not in steep]
    sums = {side: f[5 * side + 2] for side in merged}
    density = total_of([f[p] for p in rest] + list(sums.values()))
    inverse = 1.0 / density
    vel = []
    for axis in range(3):
        plus = [f[p] for p in rest if DIRS[p][axis] == 1]
        minus = [f[p] for p in rest if DIRS[p][axis] == -1]
        if axis == 1:
            plus += [f[5 * side + 3] for side in merged]
        if axis == 2:
            for side in merged:
                (minus if side else plus).append(sums[side])
        vel.append((total_of(plus) - total_of(minus)) * inverse)
    return density, vel


def collided(f, relax):
    density, (vx, vy, vz) = fields(f)
    base = 1.0 - 1.5 * (vx * vx + vy * vy + vz * vz)
    keep = 1.0 - relax
    scale = relax * density
    result = [None] * 19
    for p, c in enumerate(DIRS):
        if result[p] is not None:
            continue
        size = sum(abs(e) for e in c)
        if size == 0:
            result[p] = keep * f[p] + (scale * (1.0 / 3.0)) * base
            continue
        along = total_of(v if e == 1 else -v for e, v in zip(c, (vx, vy, vz)) if e)
        weight = scale * (1.0 / 18.0 if size == 1 else 1.0 / 36.0)
        even = weight * (base + 4.5 * (along * along))
        odd = weight * (3.0 * along)
        q = DIRS.index(tuple(-e for e in c))
        result[p] = keep * f[p] + (even + odd)
        result[q] = keep * f[q] + (even - odd)
    return result


def lane_gather(table, index):
    return jnp.take_along_axis(table, index, axis=1, mode="promise_in_bounds")


def thirds(value):
    parts = []
    for _ in range(3):
        piece = value.astype(jnp.bfloat16).astype(jnp.float32)
        parts.append(piece)
        value = value - piece
    return parts


def by_hits(data, hits, dims):
    return lax.dot_general(
        data.astype(jnp.bfloat16), hits, (dims, ((), ())), preferred_element_type=jnp.float32
    )


def coupled_kernel(
    n_slab,
    n_md,
    f_hbm,
    relax_hbm,
    own_hbm,
    pos_hbm,
    vel_hbm,
    nbr_hbm,
    slots_hbm,
    out_ref,
    pos_out,
    vel_out,
    cell_out,
    f_ref,
    relax_ref,
    own_ref,
    pos_ref,
    vel_ref,
    nbr_ref,
    slots_ref,
    load_sem,
    post,
    rows_out,
    rows_in,
    edge_out,
    edge_in,
    mean_ref,
    at,
    pull,
    steps_at,
    pairs_at,
    span,
    data,
    hits,
    placed,
    tgt,
    table,
    blocks_out,
    blocks_in,
    send,
    recv,
    late,
    swap_send,
    swap_recv,
):
    cz, cx, ny = relax_ref.shape
    top_z = cz - 1
    cells = cz * cx
    entries, atoms = nbr_ref.shape
    groups = atoms // 128
    slot_count = hits.shape[0]
    devices = n_slab * n_md
    cap = slot_count // devices
    parts = parts_of(cx)
    chunks = len(parts)
    outer = [[low for low, _ in parts].index(0), [high for _, high in parts].index(cx)]
    slab, md = lax.axis_index("slab"), lax.axis_index("md")
    me = slab * n_md + md

    def wrapped(value, size):
        return jnp.where(value >= size, value - size, value)

    above, below = wrapped(slab + 1, n_slab), wrapped(slab + n_slab - 1, n_slab)
    right, left = wrapped(md + 1, n_md), wrapped(md + n_md - 1, n_md)
    barrier = pltpu.get_barrier_semaphore()

    def peer_of(k):
        return wrapped(slab + k // n_md, n_slab), wrapped(md + k % n_md, n_md)

    def source_of(k):
        return wrapped(slab + n_slab - k // n_md, n_slab), wrapped(md + n_md - k % n_md, n_md)

    loads = []

    def fetch(src, dst):
        made = pltpu.make_async_copy(src, dst, load_sem.at[len(loads)])
        made.start()
        loads.append(made)
        return made

    f_parts = []
    for low, high in parts[:2] + [(8, cx - 8)]:
        if low < high:
            here = pl.ds(low, high - low)
            f_parts.append(fetch(f_hbm.at[:, :, here, :], f_ref.at[:, :, here, :]))
        if len(f_parts) == 1:
            relax_part = fetch(relax_hbm, relax_ref)
    if max(n_slab // 2, n_md // 2) <= LB_STEPS:
        near = {(a % n_slab) * n_md + b % n_md for a in (-1, 0, 1) for b in (-1, 0, 1)}
        greeted = sorted(near - {0})
    else:
        greeted = list(range(1, devices))
    for k in greeted:
        pl.semaphore_signal(barrier, inc=1, device_id=peer_of(k), device_id_type=MESH)
    pos_parts = [fetch(pos_hbm, pos_ref), fetch(vel_hbm, vel_ref), fetch(nbr_hbm, nbr_ref)]
    slots_part = fetch(slots_hbm, slots_ref)
    own_part = fetch(own_hbm, own_ref)

    def load(step, z, x0):
        if step == 0:
            return [f_ref[ORDER[p], z, pl.ds(x0, 8), :] for p in range(19)]
        return [
            post[step - 1, p, z + 1 - c[2], pl.ds(x0 + (8 - c[0]), 8), :]
            for p, c in enumerate(DIRS)
        ]

    def collide_chunk(step, z, part):
        for x0 in range(*parts[part], 8):
            done = collided(load(step, z, x0), relax_ref[z, pl.ds(x0, 8), :])
            done = [
                done[p] if c[1] == 0 else pltpu.roll(done[p], c[1] % ny, axis=1)
                for p, c in enumerate(DIRS)
            ]
            for side, edge in enumerate((top_z, 0)):
                if step == LB_STEPS - 1 and z == edge:
                    straight, ahead, back = (done[p] for p in STEEP[side])
                    done[5 * side + 2 : 5 * side + 5] = [
                        straight + (ahead + back),
                        ahead - back,
                        straight,
                    ]
            for p in range(19):
                post[step, p, z + 1, pl.ds(x0 + 8, 8), :] = done[p]

    def copy(step, kind, slot, src, dst, peer):
        pltpu.make_async_remote_copy(
            src_ref=src,
            dst_ref=dst,
            send_sem=send.at[kind],
            recv_sem=recv.at[step % 2, slot],
            device_id=peer,
            device_id_type=MESH,
        ).start()

    def whole(src, dst, send_sem, recv_sem):
        return pltpu.make_async_remote_copy(
            src_ref=src,
            dst_ref=dst,
            send_sem=send_sem,
            recv_sem=recv_sem,
            device_id=(above, md),
            device_id_type=MESH,
        )

    arrived = set()

    def arrive(step, slot, ref):
        if (step, slot) in arrived:
            return False
        arrived.add((step, slot))
        whole(ref, ref, send.at[0], recv.at[step % 2, slot]).wait_recv()
        return True

    def save_face(step, z, side):
        row = (7 + cx, 8)[side]
        for j, p in enumerate(FACES[side]):
            rows_out[step, side, z, j, :] = post[step, p, z + 1, row, :]

    def send_face(step, side):
        copy(
            step,
            0,
            side,
            rows_out.at[step, side],
            rows_in.at[step, side],
            (slab, (right, left)[side]),
        )

    EDGES = [[DIRS.index((x, 0, z)) for z in (-1, 1)] for x in (1, -1)]

    def send_edge(step, rising, side):
        z, peer = (top_z, above) if rising else (0, below)
        row = (7 + cx, 8)[side]
        edge_out[step, side, int(rising), 0, :] = post[step, EDGES[side][int(rising)], z + 1, row, :]
        copy(
            step,
            1,
            2 + side,
            edge_out.at[step, side, int(rising)],
            edge_in.at[step, side, int(rising)],
            (peer, (right, left)[side]),
        )

    def send_plane(step, rising, part):
        z, slot, peer = (top_z, 0, above) if rising else (0, cz + 1, below)
        span = pl.ds(0 if rising else 5, 4 if step == LB_STEPS - 1 else 5)
        low, high = parts[part]
        here = pl.ds(8 + low, high - low)
        copy(
            step,
            3 if step == LB_STEPS - 1 else 2,
            4 + part,
            post.at[step, span, z + 1, here, :],
            post.at[step, span, slot, here, :],
            (peer, md),
        )

    def need(step, part):
        for side in range(2):
            if part != outer[side] or not arrive(step, side, rows_in.at[step, side]):
                continue
            row = (7, 8 + cx)[side]
            for j, p in enumerate(FACES[side]):
                for z in range(cz):
                    post[step, p, z + 1, row, :] = rows_in[step, side, z, j, :]
            arrive(step, 2 + side, edge_in.at[step, side])
            for rising in range(2):
                slot = 0 if rising else cz + 1
                post[step, EDGES[side][rising], slot, row, :] = edge_in[step, side, rising, 0, :]
        low, high = parts[part]
        for other, (first, last) in enumerate(parts):
            if first <= high and last >= low:
                here = pl.ds(8 + first, last - first)
                span = pl.ds(0, 8 if step == LB_STEPS - 1 else 10)
                arrive(step, 4 + other, post.at[step, span, 0, here, :])

    def send_chunk(step, rising, part):
        z = top_z if rising else 0
        for side in range(2):
            if part == outer[1 - side]:
                save_face(step, z, side)
                send_edge(step, rising, side)
        send_plane(step, rising, part)

    def lattice_step(step):
        for part in range(chunks):
            if step == 0:
                if part < len(f_parts):
                    f_parts[part].wait()
                if part == 0:
                    relax_part.wait()
            if step:
                with mark("need"):
                    need(step - 1, part)
            for rising in (True, False):
                with mark("collide"):
                    collide_chunk(step, top_z if rising else 0, part)
                if step or part:
                    send_chunk(step, rising, part)
            for z in range(1, top_z):
                collide_chunk(step, z, part)
                for side in range(2):
                    if part == outer[1 - side]:
                        save_face(step, z, side)
            if step == 0 and part == 0:
                with mark("barrier"):
                    pl.semaphore_wait(barrier, len(greeted))
                for rising in (True, False):
                    send_chunk(step, rising, part)
            for side in range(2):
                if part == outer[1 - side]:
                    send_face(step, side)

    def pair_forces():
        for g in range(groups):
            mine = [jnp.broadcast_to(at[c, pl.ds(g, 1), :], (8, 128)) for c in range(3)]
            sums = [jnp.zeros((8, 128), jnp.float32)] * 3
            for k in range(0, entries, 8):
                index = nbr_ref[pl.ds(k, 8), pl.ds(g * 128, 128)]
                lane, row = index & 127, index >> 7
                found = [None] * 3
                for h in range(groups):
                    pick = row == h
                    for c in range(3):
                        line = jnp.broadcast_to(at[c, pl.ds(h, 1), :], (8, 128))
                        value = lane_gather(line, lane)
                        found[c] = value if h == 0 else jnp.where(pick, value, found[c])
                gap = [found[c] - mine[c] for c in range(3)]
                weight = jnp.exp(-0.5 * (gap[0] * gap[0] + gap[1] * gap[1] + gap[2] * gap[2]))
                sums = [sums[c] + gap[c] * weight for c in range(3)]
            for c in range(3):
                pull[c, pl.ds(g, 1), :] = jnp.sum(sums[c], axis=0, keepdims=True)

    half = groups // 2
    levels = 65535.0
    most_pull = 0.6066

    def extreme(value, pick):
        return jnp.broadcast_to(pick(pick(value, axis=0, keepdims=True), axis=1, keepdims=True), (1, 128))

    def prepare_span():
        places = jnp.concatenate([at[c] for c in range(3)], axis=0)
        speeds = jnp.concatenate([at[3 + c] for c in range(3)], axis=0)
        span[pl.ds(0, 1), :] = extreme(places, jnp.min)
        span[pl.ds(1, 1), :] = extreme(places, jnp.max)
        span[pl.ds(2, 1), :] = extreme(jnp.abs(speeds), jnp.max)

    def bound_span(blocks):
        per = 128 // cap
        zone = lax.broadcasted_iota(jnp.int32, (8, 128), 1) // cap
        last = zone == lax.rem(lax.rem(me, per) + 3, per)
        largest = smallest = None
        strength = jnp.zeros((8, 128), jnp.float32)
        for block in blocks:
            strength = jnp.maximum(strength, jnp.where(last, 0.0, jnp.abs(block)))
            rate = jnp.where(last, friction * block, 0.0)
            largest = rate if largest is None else jnp.maximum(largest, rate)
            smallest = rate if smallest is None else jnp.minimum(smallest, rate)
        far, least, most = extreme(strength, jnp.max), extreme(smallest, jnp.min), extreme(largest, jnp.max)
        tame = (least >= 0.0) & (time_step * most <= 1.0)
        strong = time_step * jnp.maximum(jnp.abs(least), jnp.abs(most))
        low, high, speed = (span[pl.ds(i, 1), :] for i in range(3))
        for step in range(1, MD_STEPS):
            speed = jnp.where(tame, jnp.maximum(speed, far), speed + strong * (speed + far))
            speed = (speed + time_step * pair_strength * entries * most_pull) * 1.0001
            low, high = low - time_step * speed, high + time_step * speed
            width = jnp.maximum(high - low, 1e-20)
            span[pl.ds(4 + 2 * step, 1), :] = low
            span[pl.ds(5 + 2 * step, 1), :] = width * (1.0 / levels)

    def coarse_forces(step):
        low = span[pl.ds(4 + 2 * step, 1), :]
        unit = span[pl.ds(5 + 2 * step, 1), :]
        per_unit = 1.0 / unit
        for c in range(3):
            level = jnp.clip((at[c] - low) * per_unit + 0.5, 0.0, levels).astype(jnp.int32)
            steps_at[c] = level
            pairs_at[c] = level[:half] | (level[half:] << 16)
        decay = (-0.5 * 1.4426950408889634) * (unit * unit)
        for g in range(groups):
            mine = [
                jnp.broadcast_to(steps_at[c, pl.ds(g, 1), :].astype(jnp.float32), (8, 128)) for c in range(3)
            ]
            sums = [jnp.zeros((8, 128), jnp.float32)] * 3
            for k in range(0, entries, 8):
                index = nbr_ref[pl.ds(k, 8), pl.ds(g * 128, 128)]
                lane, row = index & 127, index >> 7
                upper = row >= half
                row = jnp.where(upper, row - half, row)
                shift = jnp.where(upper, 16, 0)
                found = [None] * 3
                for h in range(half):
                    pick = row == h
                    for c in range(3):
                        line = jnp.broadcast_to(pairs_at[c, pl.ds(h, 1), :], (8, 128))
                        value = lane_gather(line, lane)
                        found[c] = value if h == 0 else jnp.where(pick, value, found[c])
                gap = [
                    (lax.shift_right_logical(found[c], shift) & 65535).astype(jnp.float32) - mine[c]
                    for c in range(3)
                ]
                weight = jnp.exp2((gap[0] * gap[0] + gap[1] * gap[1] + gap[2] * gap[2]) * decay)
                sums = [sums[c] + gap[c] * weight for c in range(3)]
            for c in range(3):
                pull[c, pl.ds(g, 1), :] = jnp.sum(sums[c], axis=0, keepdims=True) * unit

    def prepare_particles():
        for part in pos_parts:
            part.wait()
        for g in range(groups):
            here = pl.ds(g * 128, 128)
            for c in range(3):
                at[c, pl.ds(g, 1), :] = pos_ref[pl.ds(c, 1), here]
                at[3 + c, pl.ds(g, 1), :] = vel_ref[pl.ds(c, 1), here]
        prepare_span()
        pair_forces()

    def prepare_hits():
        slots_part.wait()
        data[...] = jnp.ones(data.shape, jnp.float32)
        tgt[...] = jnp.zeros(tgt.shape, jnp.float32)
        table[...] = jnp.zeros(table.shape, jnp.float32)
        for g in range(groups):
            label = lax.broadcasted_iota(jnp.int32, (slot_count, 128), 0)
            same = label == slots_ref[pl.ds(g, 1), :]
            hits[:, pl.ds(g * 128, 128)] = jnp.where(same, 1.0, 0.0).astype(jnp.bfloat16)

    def prepare_routes():
        own_part.wait()
        top = own_ref.shape[1]
        owner = [
            jnp.concatenate([own_ref[z, pl.ds(k, 1), :] for z in range(cz)], axis=1)
            for k in range(top)
        ]
        label = lax.broadcasted_iota(jnp.int32, (devices, cells), 0)
        owned = [jnp.where(label == owner[k], 1.0, 0.0) for k in range(top)]
        earlier = lax.broadcasted_iota(jnp.int32, (cells, cells), 0) < lax.broadcasted_iota(
            jnp.int32, (cells, cells), 1
        )
        before = by_hits(
            total_of(owned), jnp.where(earlier, 1.0, 0.0).astype(jnp.bfloat16), ((1,), (0,))
        )
        start = (label * cap).astype(jnp.float32)
        place = lax.broadcasted_iota(jnp.int32, (slot_count, cells), 0).astype(jnp.float32)
        filled = jnp.zeros((slot_count, cells), jnp.float32)
        for k in range(top):
            spot = jnp.sum((before + start) * owned[k], axis=0, keepdims=True)
            filled = filled + jnp.where(place == spot, 1.0, 0.0)
            before = before + owned[k]
        placed[...] = filled.astype(jnp.bfloat16)

    def swap(turn, values, meanwhile):
        per = 128 // cap
        zone = lax.broadcasted_iota(jnp.int32, (4, 128), 1) // cap
        step = lax.broadcasted_iota(jnp.int32, (4, 128), 0)
        for h in range(slot_count // 128):
            turned = pltpu.roll(
                values[:, h * 128 : (h + 1) * 128], 0, axis=1, stride=cap, stride_axis=0
            )
            for j in range(per):
                own = zone == (step + j) % per
                blocks_out[turn, h * per + j] = jnp.sum(
                    jnp.where(own, turned, 0.0), axis=0, keepdims=True
                )
        with mark("begin"):
            for k in sorted(range(1, devices), key=lambda k: -min(k // n_md, n_slab - k // n_md)):
                peer = peer_of(k)
                pltpu.make_async_remote_copy(
                    src_ref=blocks_out.at[turn, peer[0] * n_md + peer[1]],
                    dst_ref=blocks_in.at[turn, me],
                    send_sem=swap_send.at[turn],
                    recv_sem=swap_recv.at[turn],
                    device_id=peer,
                    device_id_type=MESH,
                ).start()
        blocks_in[turn, me] = blocks_out[turn, me]
        meanwhile()
        others = pl.ds(1, devices - 1)
        everyone = whole(
            blocks_out.at[turn, others],
            blocks_in.at[turn, others],
            swap_send.at[turn],
            swap_recv.at[turn],
        )
        with mark("landed"):
            everyone.wait_recv()
        place = lax.rem(me, per)
        zone = lax.broadcasted_iota(jnp.int32, (8, 128), 1) // cap
        step = lax.broadcasted_iota(jnp.int32, (8, 128), 0)
        lines, blocks = [], []
        for h in range(slot_count // 128):
            rows = [jnp.zeros((1, 128), jnp.float32)] * 4
            for b in range(per // 8):
                block = blocks_in[turn, pl.ds(h * per + b * 8, 8), 0, :]
                blocks.append(block)
                turned = pltpu.roll(block, 0, axis=1, stride=cap, stride_axis=0)
                for c in range(4):
                    own = zone == lax.rem(step + (c + place), per)
                    row = jnp.sum(jnp.where(own, turned, 0.0), axis=0, keepdims=True)
                    shift = b * 8 * cap
                    rows[c] = rows[c] + (row if shift == 0 else pltpu.roll(row, shift, axis=1))
            lines.append(rows)
        return lines, blocks, everyone.wait_send

    lattice_step(0)
    with mark("prep_part"):
        prepare_particles()
    lattice_step(1)
    with mark("hits"):
        prepare_hits()
    lattice_step(2)
    with mark("routes"):
        prepare_routes()
    for step in range(3, LB_STEPS):
        lattice_step(step)

    def merged_of(z):
        return [side for side, edge in enumerate((0, top_z)) if z == edge]

    def finish_chunk(z, part):
        for x0 in range(*parts[part], 8):
            density, vel = merged_fields(load(LB_STEPS, z, x0), merged_of(z))
            for c, value in enumerate((*vel, density)):
                mean_ref[c, pl.ds(x0 + z * cx, 8), :] = value

    late_part = post.at[LB_STEPS - 1, pl.ds(0, 2), 0, pl.ds(8, cx), :]

    def send_rest():
        for rising in (True, False):
            z, slot, peer = (top_z, 0, above) if rising else (0, cz + 1, below)
            here = (LB_STEPS - 1, 4 if rising else 9)
            pltpu.make_async_remote_copy(
                src_ref=post.at[here[0], here[1], z + 1, pl.ds(8, cx), :],
                dst_ref=post.at[here[0], here[1], slot, pl.ds(8, cx), :],
                send_sem=late.at[0],
                recv_sem=late.at[1],
                device_id=(peer, md),
                device_id_type=MESH,
            ).start()

    def put_populations():
        whole(late_part, late_part, late.at[0], late.at[1]).wait_recv()
        for z in range(cz):
            for x0 in range(0, cx, 8):
                f = load(LB_STEPS, z, x0)
                for side in merged_of(z):
                    both, apart, straight = f[5 * side + 2 : 5 * side + 5]
                    both = both - straight
                    values = (straight, 0.5 * (both + apart), 0.5 * (both - apart))
                    for p, value in zip(STEEP[side], values):
                        f[p] = value
                for p in range(19):
                    out_ref[ORDER[p], z, pl.ds(x0, 8), :] = f[p]
        whole(late_part, late_part, late.at[0], late.at[1]).wait_send()

    for part in range(chunks):
        with mark("need_last"):
            need(LB_STEPS - 1, part)
        for rising in (True, False):
            finish_chunk(top_z if rising else 0, part)
        for z in range(1, top_z):
            finish_chunk(z, part)

    with mark("mean"):
        for c in range(4):
            scale = (velocity_scale if c < 3 else 1.0) / ny
            mean = jnp.sum(mean_ref[c].T, axis=0, keepdims=True) * scale
            for part, piece in enumerate(thirds(mean)):
                tgt[pl.ds(part * 4 + c, 1), :] = piece
        sums = by_hits(tgt[...], placed[...], ((1,), (1,)))

    def lattice_sent():
        send_rest()
        for kind, ref in enumerate((rows_out, edge_out)):
            whole(ref, ref, send.at[kind], recv.at[0, 0]).wait_send()
        last = LB_STEPS - 1
        earlier = post.at[pl.ds(0, last), pl.ds(0, 10), 0, pl.ds(8, cx), :]
        whole(earlier, earlier, send.at[2], recv.at[0, 0]).wait_send()
        latest = post.at[last, pl.ds(0, 8), 0, pl.ds(8, cx), :]
        whole(latest, latest, send.at[3], recv.at[0, 0]).wait_send()

    with mark("swap0"):
        lines, blocks, sent_first = swap(0, sums[0:4] + sums[4:8] + sums[8:12], lattice_sent)

    per = 128 // cap
    slots = slots_ref[...]
    row = slots >> 7
    goal = []
    for c in range(4):
        lane = (slots + (c + lax.rem(me, per)) * cap) & 127
        value = jnp.zeros((groups, 128), jnp.float32)
        for h, line in enumerate(lines):
            spread = jnp.broadcast_to(line[c], (groups, 128))
            value = jnp.where(row == h, lane_gather(spread, lane), value)
        goal.append(value)
    rate = friction * goal[3]

    def advance():
        for c in range(3):
            vel = at[3 + c]
            force = pair_strength * pull[c] + rate * (goal[c] - vel)
            vel = vel + time_step * force
            at[3 + c] = vel
            at[c] = at[c] + time_step * vel

    def one_step(step, carry):
        with mark("pair"):
            coarse_forces(step)
        with mark("advance"):
            advance()
        return carry

    bound_span(blocks)
    advance()
    lax.fori_loop(1, MD_STEPS, one_step, 0)
    with mark("moments"):
        at[6] = at[3] * at[3] + at[4] * at[4] + at[5] * at[5]
        for c in range(4):
            for part, piece in enumerate(thirds(at[3 + c])):
                for g in range(groups):
                    data[pl.ds(part * 4 + c, 1), pl.ds(g * 128, 128)] = piece[g : g + 1, :]
        sums = by_hits(data[...], hits[...], ((1,), (1,)))
        moments = (sums[0:4] + sums[4:8] + sums[8:12]) / jnp.maximum(sums[12:13], 1.0)

    def put_particles():
        put_populations()
        sent_first()
        for g in range(groups):
            here = pl.ds(g * 128, 128)
            for c in range(3):
                pos_out[pl.ds(c, 1), here] = at[c, pl.ds(g, 1), :]
                vel_out[pl.ds(c, 1), here] = at[3 + c, pl.ds(g, 1), :]

    with mark("swap1"):
        lines, _, sent_second = swap(1, moments, put_particles)
    for h, line in enumerate(lines):
        for c in range(4):
            whole_line = pltpu.roll(line[c], 128 - lax.rem(c + lax.rem(me, per), per) * cap, axis=1)
            for part, piece in enumerate(thirds(whole_line)):
                table[pl.ds(part * 4 + c, 1), pl.ds(h * 128, 128)] = piece
    sums = by_hits(table[...], placed[...], ((1,), (0,)))
    picked = sums[0:4] + sums[4:8] + sums[8:12]
    for c in range(4):
        for z in range(cz):
            cell_out[c, pl.ds(z, 1), :] = picked[c : c + 1, z * cx : (z + 1) * cx]
    sent_second()


def put_out(*refs):
    count = len(refs) // 2
    copies = [
        pltpu.make_async_copy(refs[i], refs[count + i], refs[-1].at[i]) for i in range(count)
    ]
    for made in copies:
        made.start()
    for made in copies:
        made.wait()


def on_device(populations, relax, owners, positions, velocities, neighbours, atom_slots):
    cz, cx, ny = relax.shape
    n_slab = lax.axis_size("slab")
    n_md = lax.axis_size("md")
    devices = n_slab * n_md
    top = owners.shape[2]
    cap = cz * max(2, 2 * cx * top // devices)
    slots = devices * cap
    atoms, entries = neighbours.shape
    groups = atoms // 128
    cells = cz * cx
    chunks = len(parts_of(cx))
    vmem = pl.BlockSpec(memory_space=pltpu.VMEM)
    hbm = pl.BlockSpec(memory_space=pltpu.HBM)
    dma = pltpu.SemaphoreType.DMA
    held = [populations.shape, positions.shape, velocities.shape, (4, cz, cx)]
    args = (
        populations,
        relax,
        owners.transpose(0, 2, 1),
        positions,
        velocities,
        neighbours.T,
        atom_slots.reshape(groups, 128),
    )
    results = pl.pallas_call(
        functools.partial(coupled_kernel, n_slab, n_md),
        out_shape=tuple(pltpu.VMEM(shape, jnp.float32) for shape in held),
        in_specs=[hbm] * 7,
        out_specs=(vmem,) * 4,
        scratch_shapes=[
            pltpu.VMEM(populations.shape, jnp.float32),
            pltpu.VMEM(relax.shape, jnp.float32),
            pltpu.VMEM((cz, top, cx), jnp.int32),
            pltpu.VMEM(positions.shape, jnp.float32),
            pltpu.VMEM(velocities.shape, jnp.float32),
            pltpu.VMEM((entries, atoms), jnp.int32),
            pltpu.VMEM((groups, 128), jnp.int32),
            dma((9,)),
            pltpu.VMEM((LB_STEPS, 19, cz + 2, cx + 16, ny), jnp.float32),
            pltpu.VMEM((LB_STEPS, 2, cz, 8, ny), jnp.float32),
            pltpu.VMEM((LB_STEPS, 2, cz, 8, ny), jnp.float32),
            pltpu.VMEM((LB_STEPS, 2, 2, 1, ny), jnp.float32),
            pltpu.VMEM((LB_STEPS, 2, 2, 1, ny), jnp.float32),
            pltpu.VMEM((4, cells, ny), jnp.float32),
            pltpu.VMEM((7, groups, 128), jnp.float32),
            pltpu.VMEM((3, groups, 128), jnp.float32),
            pltpu.VMEM((3, groups, 128), jnp.int32),
            pltpu.VMEM((3, groups // 2, 128), jnp.int32),
            pltpu.VMEM((4 + 2 * MD_STEPS, 128), jnp.float32),
            pltpu.VMEM((16, atoms), jnp.float32),
            pltpu.VMEM((slots, atoms), jnp.bfloat16),
            pltpu.VMEM((slots, cells), jnp.bfloat16),
            pltpu.VMEM((16, cells), jnp.float32),
            pltpu.VMEM((16, slots), jnp.float32),
            pltpu.VMEM((2, devices, 1, 128), jnp.float32),
            pltpu.VMEM((2, devices, 1, 128), jnp.float32),
            dma((4,)),
            dma((2, 4 + chunks)),
            dma((2,)),
            dma((2,)),
            dma((2,)),
        ],
        compiler_params=pltpu.CompilerParams(
            collective_id=0, has_side_effects=True, vmem_limit_bytes=48 * 1024 * 1024
        ),
        name="coupled",
    )(*(pltpu.with_memory_space_constraint(arg, pltpu.HBM) for arg in args))
    return pl.pallas_call(
        put_out,
        out_shape=tuple(jax.ShapeDtypeStruct(shape, jnp.float32) for shape in held),
        in_specs=[vmem] * 4,
        out_specs=(hbm,) * 4,
        scratch_shapes=[dma((4,))],
        compiler_params=pltpu.CompilerParams(vmem_limit_bytes=4 * 1024 * 1024),
        name="put_out",
    )(*(pltpu.with_memory_space_constraint(part, pltpu.VMEM) for part in results))


def solution(mesh):
    return jax.shard_map(
        on_device,
        mesh=mesh,
        in_specs=(
            P(None, "slab", "md", None),
            P("slab", "md", None),
            P("slab", "md", None),
            P(None, ("slab", "md")),
            P(None, ("slab", "md")),
            P(("slab", "md"), None),
            P(("slab", "md")),
        ),
        out_specs=(
            P(None, "slab", "md", None),
            P(None, ("slab", "md")),
            P(None, ("slab", "md")),
            P(None, "slab", "md"),
        ),
        check_vma=False,
    )
```

```python
import contextlib
import functools

import jax
import jax.numpy as jnp
from jax import lax
from jax.experimental import pallas as pl
from jax.experimental.pallas import tpu as pltpu
from jax.sharding import PartitionSpec as P

LB_STEPS = 4
MD_STEPS = 5

ORDER = [11, 14, 5, 15, 18, 12, 13, 6, 16, 17, 0, 1, 2, 3, 4, 7, 8, 9, 10]
lattice_dirs = [
    (0, 0, 0),
    (1, 0, 0),
    (-1, 0, 0),
    (0, 1, 0),
    (0, -1, 0),
    (0, 0, 1),
    (0, 0, -1),
    (1, 1, 0),
    (-1, -1, 0),
    (1, -1, 0),
    (-1, 1, 0),
    (1, 0, 1),
    (-1, 0, -1),
    (1, 0, -1),
    (-1, 0, 1),
    (0, 1, 1),
    (0, -1, -1),
    (0, 1, -1),
    (0, -1, 1),
]
DIRS = [lattice_dirs[i] for i in ORDER]
FACES = [[p for p in range(19) if DIRS[p][0] == 1], [p for p in range(19) if DIRS[p][0] == -1]]
STEEP = [[DIRS.index((0, y, z)) for y in (0, 1, -1)] for z in (1, -1)]
velocity_scale = 10.0
pair_strength = 0.5
friction = 2.0
time_step = 0.1
MESH = pl.DeviceIdType.MESH


def parts_of(cx):
    edges = list(range(0, cx + 1, 8))
    parts = list(zip(edges[:-1], edges[1:]))
    order = []
    while parts:
        order.append(parts.pop(0))
        if parts:
            order.append(parts.pop())
    return order


def mark(name):
    return contextlib.nullcontext()


def total_of(terms):
    terms = list(terms)
    while len(terms) > 1:
        terms = [a + b for a, b in zip(terms[::2], terms[1::2])] + (
            [terms[-1]] if len(terms) % 2 else []
        )
    return terms[0]


def fields(f):
    density = total_of(f)
    inverse = 1.0 / density
    vel = []
    for axis in range(3):
        plus = total_of(f[p] for p in range(19) if DIRS[p][axis] == 1)
        minus = total_of(f[p] for p in range(19) if DIRS[p][axis] == -1)
        vel.append((plus - minus) * inverse)
    return density, vel


def merged_fields(f, merged):
    steep = [p for side in merged for p in STEEP[side]]
    rest = [p for p in range(19) if p not in steep]
    sums = {side: f[5 * side + 2] for side in merged}
    density = total_of([f[p] for p in rest] + list(sums.values()))
    inverse = 1.0 / density
    vel = []
    for axis in range(3):
        plus = [f[p] for p in rest if DIRS[p][axis] == 1]
        minus = [f[p] for p in rest if DIRS[p][axis] == -1]
        if axis == 1:
            plus += [f[5 * side + 3] for side in merged]
        if axis == 2:
            for side in merged:
                (minus if side else plus).append(sums[side])
        vel.append((total_of(plus) - total_of(minus)) * inverse)
    return density, vel


def collided(f, relax):
    density, (vx, vy, vz) = fields(f)
    base = 1.0 - 1.5 * (vx * vx + vy * vy + vz * vz)
    keep = 1.0 - relax
    scale = relax * density
    result = [None] * 19
    for p, c in enumerate(DIRS):
        if result[p] is not None:
            continue
        size = sum(abs(e) for e in c)
        if size == 0:
            result[p] = keep * f[p] + (scale * (1.0 / 3.0)) * base
            continue
        along = total_of(v if e == 1 else -v for e, v in zip(c, (vx, vy, vz)) if e)
        weight = scale * (1.0 / 18.0 if size == 1 else 1.0 / 36.0)
        even = weight * (base + 4.5 * (along * along))
        odd = weight * (3.0 * along)
        q = DIRS.index(tuple(-e for e in c))
        result[p] = keep * f[p] + (even + odd)
        result[q] = keep * f[q] + (even - odd)
    return result


def lane_gather(table, index):
    return jnp.take_along_axis(table, index, axis=1, mode="promise_in_bounds")


def thirds(value):
    parts = []
    for _ in range(3):
        piece = value.astype(jnp.bfloat16).astype(jnp.float32)
        parts.append(piece)
        value = value - piece
    return parts


def by_hits(data, hits, dims):
    return lax.dot_general(
        data.astype(jnp.bfloat16), hits, (dims, ((), ())), preferred_element_type=jnp.float32
    )


def coupled_kernel(
    n_slab,
    n_md,
    f_hbm,
    relax_hbm,
    own_hbm,
    pos_hbm,
    vel_hbm,
    nbr_hbm,
    slots_hbm,
    out_ref,
    pos_out,
    vel_out,
    cell_out,
    f_ref,
    relax_ref,
    own_ref,
    pos_ref,
    vel_ref,
    nbr_ref,
    slots_ref,
    load_sem,
    post,
    rows_out,
    rows_in,
    edge_out,
    edge_in,
    mean_ref,
    at,
    pull,
    steps_at,
    pairs_at,
    span,
    data,
    hits,
    placed,
    tgt,
    table,
    blocks_out,
    blocks_in,
    send,
    recv,
    late,
    apart,
    swap_send,
    swap_recv,
):
    cz, cx, ny = relax_ref.shape
    top_z = cz - 1
    cells = cz * cx
    entries, atoms = nbr_ref.shape
    groups = atoms // 128
    slot_count = hits.shape[0]
    devices = n_slab * n_md
    cap = slot_count // devices
    parts = parts_of(cx)
    chunks = len(parts)
    outer = [[low for low, _ in parts].index(0), [high for _, high in parts].index(cx)]
    slab, md = lax.axis_index("slab"), lax.axis_index("md")
    me = slab * n_md + md

    def wrapped(value, size):
        return jnp.where(value >= size, value - size, value)

    above, below = wrapped(slab + 1, n_slab), wrapped(slab + n_slab - 1, n_slab)
    right, left = wrapped(md + 1, n_md), wrapped(md + n_md - 1, n_md)
    barrier = pltpu.get_barrier_semaphore()

    def peer_of(k):
        return wrapped(slab + k // n_md, n_slab), wrapped(md + k % n_md, n_md)

    def source_of(k):
        return wrapped(slab + n_slab - k // n_md, n_slab), wrapped(md + n_md - k % n_md, n_md)

    loads = []

    def fetch(src, dst):
        made = pltpu.make_async_copy(src, dst, load_sem.at[len(loads)])
        made.start()
        loads.append(made)
        return made

    f_parts = []
    for low, high in parts[:2] + [(8, cx - 8)]:
        if low < high:
            here = pl.ds(low, high - low)
            f_parts.append(fetch(f_hbm.at[:, :, here, :], f_ref.at[:, :, here, :]))
        if len(f_parts) == 1:
            relax_part = fetch(relax_hbm, relax_ref)
    reach = min(n_slab, n_md) > 2 and max(n_slab // 2, n_md // 2) <= LB_STEPS
    first_slab, last_slab = slab == 0, slab == n_slab - 1

    def signal(k, flag):
        pl.semaphore_signal(flag, inc=1, device_id=peer_of(k), device_id_type=MESH)

    if reach:
        sides = [b % n_md for b in (0, 1, -1)]
        for k in [n_md * (n_slab - 1) + b for b in sides] + sides[1:]:
            signal(k, barrier)

        @pl.when(jnp.logical_not(last_slab))
        def _():
            for b in sides:
                signal(n_md + b, barrier)
    else:
        for k in range(1, devices):
            signal(k, barrier)
    pos_parts = [fetch(pos_hbm, pos_ref), fetch(vel_hbm, vel_ref), fetch(nbr_hbm, nbr_ref)]
    slots_part = fetch(slots_hbm, slots_ref)
    own_part = fetch(own_hbm, own_ref)

    def load(step, z, x0):
        if step == 0:
            return [f_ref[ORDER[p], z, pl.ds(x0, 8), :] for p in range(19)]
        return [
            post[step - 1, p, z + 1 - c[2], pl.ds(x0 + (8 - c[0]), 8), :]
            for p, c in enumerate(DIRS)
        ]

    def collide_chunk(step, z, part):
        for x0 in range(*parts[part], 8):
            done = collided(load(step, z, x0), relax_ref[z, pl.ds(x0, 8), :])
            done = [
                done[p] if c[1] == 0 else pltpu.roll(done[p], c[1] % ny, axis=1)
                for p, c in enumerate(DIRS)
            ]
            for side, edge in enumerate((top_z, 0)):
                if step == LB_STEPS - 1 and z == edge:
                    straight, ahead, back = (done[p] for p in STEEP[side])
                    done[5 * side + 2 : 5 * side + 5] = [
                        straight + (ahead + back),
                        ahead - back,
                        straight,
                    ]
            for p in range(19):
                post[step, p, z + 1, pl.ds(x0 + 8, 8), :] = done[p]

    def copy(step, kind, slot, src, dst, peer):
        pltpu.make_async_remote_copy(
            src_ref=src,
            dst_ref=dst,
            send_sem=send.at[kind],
            recv_sem=recv.at[step % 2, slot],
            device_id=peer,
            device_id_type=MESH,
        ).start()

    def whole(src, dst, send_sem, recv_sem):
        return pltpu.make_async_remote_copy(
            src_ref=src,
            dst_ref=dst,
            send_sem=send_sem,
            recv_sem=recv_sem,
            device_id=(above, md),
            device_id_type=MESH,
        )

    arrived = set()

    def arrive(step, slot, ref):
        if (step, slot) in arrived:
            return False
        arrived.add((step, slot))
        whole(ref, ref, send.at[0], recv.at[step % 2, slot]).wait_recv()
        return True

    def save_face(step, z, side):
        row = (7 + cx, 8)[side]
        for j, p in enumerate(FACES[side]):
            rows_out[step, side, z, j, :] = post[step, p, z + 1, row, :]

    def send_face(step, side):
        copy(
            step,
            0,
            side,
            rows_out.at[step, side],
            rows_in.at[step, side],
            (slab, (right, left)[side]),
        )

    EDGES = [[DIRS.index((x, 0, z)) for z in (-1, 1)] for x in (1, -1)]

    def send_edge(step, rising, side):
        z, peer = (top_z, above) if rising else (0, below)
        row = (7 + cx, 8)[side]
        edge_out[step, side, int(rising), 0, :] = post[step, EDGES[side][int(rising)], z + 1, row, :]
        copy(
            step,
            1,
            2 + side,
            edge_out.at[step, side, int(rising)],
            edge_in.at[step, side, int(rising)],
            (peer, (right, left)[side]),
        )

    def send_plane(step, rising, part):
        z, slot, peer = (top_z, 0, above) if rising else (0, cz + 1, below)
        span = pl.ds(0 if rising else 5, 4 if step == LB_STEPS - 1 else 5)
        low, high = parts[part]
        here = pl.ds(8 + low, high - low)
        copy(
            step,
            3 if step == LB_STEPS - 1 else 2,
            4 + part,
            post.at[step, span, z + 1, here, :],
            post.at[step, span, slot, here, :],
            (peer, md),
        )

    def need(step, part):
        for side in range(2):
            if part != outer[side] or not arrive(step, side, rows_in.at[step, side]):
                continue
            row = (7, 8 + cx)[side]
            for j, p in enumerate(FACES[side]):
                for z in range(cz):
                    post[step, p, z + 1, row, :] = rows_in[step, side, z, j, :]
            arrive(step, 2 + side, edge_in.at[step, side])
            for rising in range(2):
                slot = 0 if rising else cz + 1
                post[step, EDGES[side][rising], slot, row, :] = edge_in[step, side, rising, 0, :]
        low, high = parts[part]
        for other, (first, last) in enumerate(parts):
            if first <= high and last >= low:
                here = pl.ds(8 + first, last - first)
                span = pl.ds(0, 8 if step == LB_STEPS - 1 else 10)
                arrive(step, 4 + other, post.at[step, span, 0, here, :])

    def save_faces(step, z, part):
        for side in range(2):
            if part == outer[1 - side]:
                save_face(step, z, side)

    def send_blocks(step, rising, part):
        for side in range(2):
            if part == outer[1 - side]:
                send_edge(step, rising, side)
        send_plane(step, rising, part)

    def send_chunk(step, rising, part):
        save_faces(step, top_z if rising else 0, part)
        send_blocks(step, rising, part)

    def send_first(rising, part):
        save_faces(0, top_z if rising else 0, part)
        if rising or not reach:
            send_blocks(0, rising, part)
        else:
            pl.when(jnp.logical_not(first_slab))(lambda: send_blocks(0, rising, part))

    def send_late_falling():
        pl.semaphore_wait(apart, 3)
        for part in range(chunks):
            send_blocks(0, False, part)

    def lattice_step(step):
        for part in range(chunks):
            if step == 0:
                if part < len(f_parts):
                    f_parts[part].wait()
                if part == 0:
                    relax_part.wait()
            if step:
                with mark("need"):
                    need(step - 1, part)
            for rising in (True, False):
                with mark("collide"):
                    collide_chunk(step, top_z if rising else 0, part)
                if step:
                    send_chunk(step, rising, part)
                elif part:
                    send_first(rising, part)
            for z in range(1, top_z):
                collide_chunk(step, z, part)
                for side in range(2):
                    if part == outer[1 - side]:
                        save_face(step, z, side)
            if step == 0 and part == 0:
                with mark("barrier"):
                    expected = jnp.where(first_slab, 5, 8) if reach else devices - 1
                    pl.semaphore_wait(barrier, expected)
                if reach:

                    @pl.when(last_slab)
                    def _():
                        for b in sides:
                            signal(n_md + b, apart)

                for rising in (True, False):
                    send_first(rising, part)
            for side in range(2):
                if part == outer[1 - side]:
                    send_face(step, side)

    def pair_forces():
        for g in range(groups):
            mine = [jnp.broadcast_to(at[c, pl.ds(g, 1), :], (8, 128)) for c in range(3)]
            sums = [jnp.zeros((8, 128), jnp.float32)] * 3
            for k in range(0, entries, 8):
                index = nbr_ref[pl.ds(k, 8), pl.ds(g * 128, 128)]
                lane, row = index & 127, index >> 7
                found = [None] * 3
                for h in range(groups):
                    pick = row == h
                    for c in range(3):
                        line = jnp.broadcast_to(at[c, pl.ds(h, 1), :], (8, 128))
                        value = lane_gather(line, lane)
                        found[c] = value if h == 0 else jnp.where(pick, value, found[c])
                gap = [found[c] - mine[c] for c in range(3)]
                weight = jnp.exp(-0.5 * (gap[0] * gap[0] + gap[1] * gap[1] + gap[2] * gap[2]))
                sums = [sums[c] + gap[c] * weight for c in range(3)]
            for c in range(3):
                pull[c, pl.ds(g, 1), :] = jnp.sum(sums[c], axis=0, keepdims=True)

    half = groups // 2
    levels = 65535.0
    most_pull = 0.6066

    def extreme(value, pick):
        return jnp.broadcast_to(pick(pick(value, axis=0, keepdims=True), axis=1, keepdims=True), (1, 128))

    def prepare_span():
        places = jnp.concatenate([at[c] for c in range(3)], axis=0)
        speeds = jnp.concatenate([at[3 + c] for c in range(3)], axis=0)
        span[pl.ds(0, 1), :] = extreme(places, jnp.min)
        span[pl.ds(1, 1), :] = extreme(places, jnp.max)
        span[pl.ds(2, 1), :] = extreme(jnp.abs(speeds), jnp.max)

    def bound_span(blocks):
        per = 128 // cap
        zone = lax.broadcasted_iota(jnp.int32, (8, 128), 1) // cap
        last = zone == lax.rem(lax.rem(me, per) + 3, per)
        largest = smallest = None
        strength = jnp.zeros((8, 128), jnp.float32)
        for block in blocks:
            strength = jnp.maximum(strength, jnp.where(last, 0.0, jnp.abs(block)))
            rate = jnp.where(last, friction * block, 0.0)
            largest = rate if largest is None else jnp.maximum(largest, rate)
            smallest = rate if smallest is None else jnp.minimum(smallest, rate)
        far, least, most = extreme(strength, jnp.max), extreme(smallest, jnp.min), extreme(largest, jnp.max)
        tame = (least >= 0.0) & (time_step * most <= 1.0)
        strong = time_step * jnp.maximum(jnp.abs(least), jnp.abs(most))
        low, high, speed = (span[pl.ds(i, 1), :] for i in range(3))
        for step in range(1, MD_STEPS):
            speed = jnp.where(tame, jnp.maximum(speed, far), speed + strong * (speed + far))
            speed = (speed + time_step * pair_strength * entries * most_pull) * 1.0001
            low, high = low - time_step * speed, high + time_step * speed
            width = jnp.maximum(high - low, 1e-20)
            span[pl.ds(4 + 2 * step, 1), :] = low
            span[pl.ds(5 + 2 * step, 1), :] = width * (1.0 / levels)

    def coarse_forces(step):
        low = span[pl.ds(4 + 2 * step, 1), :]
        unit = span[pl.ds(5 + 2 * step, 1), :]
        per_unit = 1.0 / unit
        for c in range(3):
            level = jnp.clip((at[c] - low) * per_unit + 0.5, 0.0, levels).astype(jnp.int32)
            steps_at[c] = level
            pairs_at[c] = level[:half] | (level[half:] << 16)
        decay = (-0.5 * 1.4426950408889634) * (unit * unit)
        for g in range(groups):
            mine = [
                jnp.broadcast_to(steps_at[c, pl.ds(g, 1), :].astype(jnp.float32), (8, 128)) for c in range(3)
            ]
            sums = [jnp.zeros((8, 128), jnp.float32)] * 3
            for k in range(0, entries, 8):
                index = nbr_ref[pl.ds(k, 8), pl.ds(g * 128, 128)]
                lane, row = index & 127, index >> 7
                upper = row >= half
                row = jnp.where(upper, row - half, row)
                shift = jnp.where(upper, 16, 0)
                found = [None] * 3
                for h in range(half):
                    pick = row == h
                    for c in range(3):
                        line = jnp.broadcast_to(pairs_at[c, pl.ds(h, 1), :], (8, 128))
                        value = lane_gather(line, lane)
                        found[c] = value if h == 0 else jnp.where(pick, value, found[c])
                gap = [
                    (lax.shift_right_logical(found[c], shift) & 65535).astype(jnp.float32) - mine[c]
                    for c in range(3)
                ]
                weight = jnp.exp2((gap[0] * gap[0] + gap[1] * gap[1] + gap[2] * gap[2]) * decay)
                sums = [sums[c] + gap[c] * weight for c in range(3)]
            for c in range(3):
                pull[c, pl.ds(g, 1), :] = jnp.sum(sums[c], axis=0, keepdims=True) * unit

    def prepare_particles():
        for part in pos_parts:
            part.wait()
        for g in range(groups):
            here = pl.ds(g * 128, 128)
            for c in range(3):
                at[c, pl.ds(g, 1), :] = pos_ref[pl.ds(c, 1), here]
                at[3 + c, pl.ds(g, 1), :] = vel_ref[pl.ds(c, 1), here]
        prepare_span()
        pair_forces()

    def prepare_hits():
        slots_part.wait()
        data[...] = jnp.ones(data.shape, jnp.float32)
        tgt[...] = jnp.zeros(tgt.shape, jnp.float32)
        table[...] = jnp.zeros(table.shape, jnp.float32)
        for g in range(groups):
            label = lax.broadcasted_iota(jnp.int32, (slot_count, 128), 0)
            same = label == slots_ref[pl.ds(g, 1), :]
            hits[:, pl.ds(g * 128, 128)] = jnp.where(same, 1.0, 0.0).astype(jnp.bfloat16)

    def prepare_routes():
        own_part.wait()
        top = own_ref.shape[1]
        owner = [
            jnp.concatenate([own_ref[z, pl.ds(k, 1), :] for z in range(cz)], axis=1)
            for k in range(top)
        ]
        label = lax.broadcasted_iota(jnp.int32, (devices, cells), 0)
        owned = [jnp.where(label == owner[k], 1.0, 0.0) for k in range(top)]
        earlier = lax.broadcasted_iota(jnp.int32, (cells, cells), 0) < lax.broadcasted_iota(
            jnp.int32, (cells, cells), 1
        )
        before = by_hits(
            total_of(owned), jnp.where(earlier, 1.0, 0.0).astype(jnp.bfloat16), ((1,), (0,))
        )
        start = (label * cap).astype(jnp.float32)
        place = lax.broadcasted_iota(jnp.int32, (slot_count, cells), 0).astype(jnp.float32)
        filled = jnp.zeros((slot_count, cells), jnp.float32)
        for k in range(top):
            spot = jnp.sum((before + start) * owned[k], axis=0, keepdims=True)
            filled = filled + jnp.where(place == spot, 1.0, 0.0)
            before = before + owned[k]
        placed[...] = filled.astype(jnp.bfloat16)

    def swap(turn, values, meanwhile):
        per = 128 // cap
        zone = lax.broadcasted_iota(jnp.int32, (4, 128), 1) // cap
        step = lax.broadcasted_iota(jnp.int32, (4, 128), 0)
        for h in range(slot_count // 128):
            turned = pltpu.roll(
                values[:, h * 128 : (h + 1) * 128], 0, axis=1, stride=cap, stride_axis=0
            )
            for j in range(per):
                own = zone == (step + j) % per
                blocks_out[turn, h * per + j] = jnp.sum(
                    jnp.where(own, turned, 0.0), axis=0, keepdims=True
                )
        with mark("begin"):
            for k in sorted(range(1, devices), key=lambda k: -min(k // n_md, n_slab - k // n_md)):
                peer = peer_of(k)
                pltpu.make_async_remote_copy(
                    src_ref=blocks_out.at[turn, peer[0] * n_md + peer[1]],
                    dst_ref=blocks_in.at[turn, me],
                    send_sem=swap_send.at[turn],
                    recv_sem=swap_recv.at[turn],
                    device_id=peer,
                    device_id_type=MESH,
                ).start()
        blocks_in[turn, me] = blocks_out[turn, me]
        meanwhile()
        others = pl.ds(1, devices - 1)
        everyone = whole(
            blocks_out.at[turn, others],
            blocks_in.at[turn, others],
            swap_send.at[turn],
            swap_recv.at[turn],
        )
        with mark("landed"):
            everyone.wait_recv()
        place = lax.rem(me, per)
        zone = lax.broadcasted_iota(jnp.int32, (8, 128), 1) // cap
        step = lax.broadcasted_iota(jnp.int32, (8, 128), 0)
        lines, blocks = [], []
        for h in range(slot_count // 128):
            rows = [jnp.zeros((1, 128), jnp.float32)] * 4
            for b in range(per // 8):
                block = blocks_in[turn, pl.ds(h * per + b * 8, 8), 0, :]
                blocks.append(block)
                turned = pltpu.roll(block, 0, axis=1, stride=cap, stride_axis=0)
                for c in range(4):
                    own = zone == lax.rem(step + (c + place), per)
                    row = jnp.sum(jnp.where(own, turned, 0.0), axis=0, keepdims=True)
                    shift = b * 8 * cap
                    rows[c] = rows[c] + (row if shift == 0 else pltpu.roll(row, shift, axis=1))
            lines.append(rows)
        return lines, blocks, everyone.wait_send

    lattice_step(0)
    if reach:
        with mark("apart"):
            pl.when(first_slab)(send_late_falling)
    with mark("prep_part"):
        prepare_particles()
    lattice_step(1)
    with mark("hits"):
        prepare_hits()
    lattice_step(2)
    with mark("routes"):
        prepare_routes()
    for step in range(3, LB_STEPS):
        lattice_step(step)

    def merged_of(z):
        return [side for side, edge in enumerate((0, top_z)) if z == edge]

    def finish_chunk(z, part):
        for x0 in range(*parts[part], 8):
            density, vel = merged_fields(load(LB_STEPS, z, x0), merged_of(z))
            for c, value in enumerate((*vel, density)):
                mean_ref[c, pl.ds(x0 + z * cx, 8), :] = value

    late_part = post.at[LB_STEPS - 1, pl.ds(0, 2), 0, pl.ds(8, cx), :]

    def send_rest():
        for rising in (True, False):
            z, slot, peer = (top_z, 0, above) if rising else (0, cz + 1, below)
            here = (LB_STEPS - 1, 4 if rising else 9)
            pltpu.make_async_remote_copy(
                src_ref=post.at[here[0], here[1], z + 1, pl.ds(8, cx), :],
                dst_ref=post.at[here[0], here[1], slot, pl.ds(8, cx), :],
                send_sem=late.at[0],
                recv_sem=late.at[1],
                device_id=(peer, md),
                device_id_type=MESH,
            ).start()

    def put_populations():
        whole(late_part, late_part, late.at[0], late.at[1]).wait_recv()
        for z in range(cz):
            for x0 in range(0, cx, 8):
                f = load(LB_STEPS, z, x0)
                for side in merged_of(z):
                    both, apart, straight = f[5 * side + 2 : 5 * side + 5]
                    both = both - straight
                    values = (straight, 0.5 * (both + apart), 0.5 * (both - apart))
                    for p, value in zip(STEEP[side], values):
                        f[p] = value
                for p in range(19):
                    out_ref[ORDER[p], z, pl.ds(x0, 8), :] = f[p]
        whole(late_part, late_part, late.at[0], late.at[1]).wait_send()

    for part in range(chunks):
        with mark("need_last"):
            need(LB_STEPS - 1, part)
        for rising in (True, False):
            finish_chunk(top_z if rising else 0, part)
        for z in range(1, top_z):
            finish_chunk(z, part)

    with mark("mean"):
        for c in range(4):
            scale = (velocity_scale if c < 3 else 1.0) / ny
            mean = jnp.sum(mean_ref[c].T, axis=0, keepdims=True) * scale
            for part, piece in enumerate(thirds(mean)):
                tgt[pl.ds(part * 4 + c, 1), :] = piece
        sums = by_hits(tgt[...], placed[...], ((1,), (1,)))

    def lattice_sent():
        send_rest()
        for kind, ref in enumerate((rows_out, edge_out)):
            whole(ref, ref, send.at[kind], recv.at[0, 0]).wait_send()
        last = LB_STEPS - 1
        earlier = post.at[pl.ds(0, last), pl.ds(0, 10), 0, pl.ds(8, cx), :]
        whole(earlier, earlier, send.at[2], recv.at[0, 0]).wait_send()
        latest = post.at[last, pl.ds(0, 8), 0, pl.ds(8, cx), :]
        whole(latest, latest, send.at[3], recv.at[0, 0]).wait_send()

    with mark("swap0"):
        lines, blocks, sent_first = swap(0, sums[0:4] + sums[4:8] + sums[8:12], lattice_sent)

    per = 128 // cap
    slots = slots_ref[...]
    row = slots >> 7
    goal = []
    for c in range(4):
        lane = (slots + (c + lax.rem(me, per)) * cap) & 127
        value = jnp.zeros((groups, 128), jnp.float32)
        for h, line in enumerate(lines):
            spread = jnp.broadcast_to(line[c], (groups, 128))
            value = jnp.where(row == h, lane_gather(spread, lane), value)
        goal.append(value)
    rate = friction * goal[3]

    def advance():
        for c in range(3):
            vel = at[3 + c]
            force = pair_strength * pull[c] + rate * (goal[c] - vel)
            vel = vel + time_step * force
            at[3 + c] = vel
            at[c] = at[c] + time_step * vel

    def one_step(step, carry):
        with mark("pair"):
            coarse_forces(step)
        with mark("advance"):
            advance()
        return carry

    bound_span(blocks)
    advance()
    lax.fori_loop(1, MD_STEPS, one_step, 0)
    with mark("moments"):
        at[6] = at[3] * at[3] + at[4] * at[4] + at[5] * at[5]
        for c in range(4):
            for part, piece in enumerate(thirds(at[3 + c])):
                for g in range(groups):
                    data[pl.ds(part * 4 + c, 1), pl.ds(g * 128, 128)] = piece[g : g + 1, :]
        sums = by_hits(data[...], hits[...], ((1,), (1,)))
        moments = (sums[0:4] + sums[4:8] + sums[8:12]) / jnp.maximum(sums[12:13], 1.0)

    def put_particles():
        put_populations()
        sent_first()
        for g in range(groups):
            here = pl.ds(g * 128, 128)
            for c in range(3):
                pos_out[pl.ds(c, 1), here] = at[c, pl.ds(g, 1), :]
                vel_out[pl.ds(c, 1), here] = at[3 + c, pl.ds(g, 1), :]

    with mark("swap1"):
        lines, _, sent_second = swap(1, moments, put_particles)
    for h, line in enumerate(lines):
        for c in range(4):
            whole_line = pltpu.roll(line[c], 128 - lax.rem(c + lax.rem(me, per), per) * cap, axis=1)
            for part, piece in enumerate(thirds(whole_line)):
                table[pl.ds(part * 4 + c, 1), pl.ds(h * 128, 128)] = piece
    sums = by_hits(table[...], placed[...], ((1,), (0,)))
    picked = sums[0:4] + sums[4:8] + sums[8:12]
    for c in range(4):
        for z in range(cz):
            cell_out[c, pl.ds(z, 1), :] = picked[c : c + 1, z * cx : (z + 1) * cx]
    sent_second()


def put_out(*refs):
    count = len(refs) // 2
    copies = [
        pltpu.make_async_copy(refs[i], refs[count + i], refs[-1].at[i]) for i in range(count)
    ]
    for made in copies:
        made.start()
    for made in copies:
        made.wait()


def on_device(populations, relax, owners, positions, velocities, neighbours, atom_slots):
    cz, cx, ny = relax.shape
    n_slab = lax.axis_size("slab")
    n_md = lax.axis_size("md")
    devices = n_slab * n_md
    top = owners.shape[2]
    cap = cz * max(2, 2 * cx * top // devices)
    slots = devices * cap
    atoms, entries = neighbours.shape
    groups = atoms // 128
    cells = cz * cx
    chunks = len(parts_of(cx))
    vmem = pl.BlockSpec(memory_space=pltpu.VMEM)
    hbm = pl.BlockSpec(memory_space=pltpu.HBM)
    dma = pltpu.SemaphoreType.DMA
    held = [populations.shape, positions.shape, velocities.shape, (4, cz, cx)]
    args = (
        populations,
        relax,
        owners.transpose(0, 2, 1),
        positions,
        velocities,
        neighbours.T,
        atom_slots.reshape(groups, 128),
    )
    results = pl.pallas_call(
        functools.partial(coupled_kernel, n_slab, n_md),
        out_shape=tuple(pltpu.VMEM(shape, jnp.float32) for shape in held),
        in_specs=[hbm] * 7,
        out_specs=(vmem,) * 4,
        scratch_shapes=[
            pltpu.VMEM(populations.shape, jnp.float32),
            pltpu.VMEM(relax.shape, jnp.float32),
            pltpu.VMEM((cz, top, cx), jnp.int32),
            pltpu.VMEM(positions.shape, jnp.float32),
            pltpu.VMEM(velocities.shape, jnp.float32),
            pltpu.VMEM((entries, atoms), jnp.int32),
            pltpu.VMEM((groups, 128), jnp.int32),
            dma((9,)),
            pltpu.VMEM((LB_STEPS, 19, cz + 2, cx + 16, ny), jnp.float32),
            pltpu.VMEM((LB_STEPS, 2, cz, 8, ny), jnp.float32),
            pltpu.VMEM((LB_STEPS, 2, cz, 8, ny), jnp.float32),
            pltpu.VMEM((LB_STEPS, 2, 2, 1, ny), jnp.float32),
            pltpu.VMEM((LB_STEPS, 2, 2, 1, ny), jnp.float32),
            pltpu.VMEM((4, cells, ny), jnp.float32),
            pltpu.VMEM((7, groups, 128), jnp.float32),
            pltpu.VMEM((3, groups, 128), jnp.float32),
            pltpu.VMEM((3, groups, 128), jnp.int32),
            pltpu.VMEM((3, groups // 2, 128), jnp.int32),
            pltpu.VMEM((4 + 2 * MD_STEPS, 128), jnp.float32),
            pltpu.VMEM((16, atoms), jnp.float32),
            pltpu.VMEM((slots, atoms), jnp.bfloat16),
            pltpu.VMEM((slots, cells), jnp.bfloat16),
            pltpu.VMEM((16, cells), jnp.float32),
            pltpu.VMEM((16, slots), jnp.float32),
            pltpu.VMEM((2, devices, 1, 128), jnp.float32),
            pltpu.VMEM((2, devices, 1, 128), jnp.float32),
            dma((4,)),
            dma((2, 4 + chunks)),
            dma((2,)),
            pltpu.SemaphoreType.REGULAR,
            dma((2,)),
            dma((2,)),
        ],
        compiler_params=pltpu.CompilerParams(
            collective_id=0, has_side_effects=True, vmem_limit_bytes=48 * 1024 * 1024
        ),
        name="coupled",
    )(*(pltpu.with_memory_space_constraint(arg, pltpu.HBM) for arg in args))
    return pl.pallas_call(
        put_out,
        out_shape=tuple(jax.ShapeDtypeStruct(shape, jnp.float32) for shape in held),
        in_specs=[vmem] * 4,
        out_specs=(hbm,) * 4,
        scratch_shapes=[dma((4,))],
        compiler_params=pltpu.CompilerParams(vmem_limit_bytes=4 * 1024 * 1024),
        name="put_out",
    )(*(pltpu.with_memory_space_constraint(part, pltpu.VMEM) for part in results))


def solution(mesh):
    return jax.shard_map(
        on_device,
        mesh=mesh,
        in_specs=(
            P(None, "slab", "md", None),
            P("slab", "md", None),
            P("slab", "md", None),
            P(None, ("slab", "md")),
            P(None, ("slab", "md")),
            P(("slab", "md"), None),
            P(("slab", "md")),
        ),
        out_specs=(
            P(None, "slab", "md", None),
            P(None, ("slab", "md")),
            P(None, ("slab", "md")),
            P(None, "slab", "md"),
        ),
        check_vma=False,
    )
```
